32 devices in a mesh: row: 2 (over x), col: 4 (over z), depth: 4 (over y, core).
Axes of the slice: x: 2, y: 2, z: 4, core: 2. Of those that a mesh axis runs over, the one named last changes fastest.
Arguments:
- pair: bfloat16 [768, 768, 128], P('row', 'col'), may hold values from -6 to 6
- ln_gain: float32 [128], replicated, may hold values from 0.1 to 1.9
- ln_shift: float32 [128], replicated, may hold values from -3 to 3
- proj_weight: bfloat16 [128, 512], replicated, may hold values from -0.5 to 0.5
- proj_bias: float32 [512], replicated, may hold values from -3 to 3
- gate_weight: bfloat16 [128, 128], replicated, may hold values from -0.5 to 0.5
- gate_bias: float32 [128], replicated, may hold values from -3 to 3
- out_gain: float32 [128], replicated, may hold values from 0.1 to 1.9
- out_shift: float32 [128], replicated, may hold values from -3 to 3
- out_weight: bfloat16 [128, 128], replicated, may hold values from -0.5 to 0.5
- out_bias: float32 [128], replicated, may hold values from -3 to 3
Outputs:
- update: bfloat16 [768, 768, 128], P('row', 'col')
The draws below stay inside these ranges and needn't reach their ends.
All inputs are finite; a program needn't handle non-finite values.
Results may differ from the reference program's by a relative error of at most 0.0051.
Values may be sent and summed in bfloat16 or wider, within the bound.
A program may use at most 256 MiB of HBM per device.

```python
import jax
import jax.numpy as jnp
from jax import lax

C = 128
HID = 128
RES = 768


def block_levels(rng, dims, split, low, largest):
    level, own = 1.0, jax.random.fold_in(rng, 6)
    for position, blocks in split:
        heights = jnp.exp(jax.random.uniform(jax.random.fold_in(own, position), (blocks,), jnp.float32, low / len(split), largest / len(split)))
        level = level * jnp.repeat(heights, dims[position] // blocks).reshape([-1 if axis == position else 1 for axis in range(len(dims))])
    return level


def gaussian(key, shape, scale, limit, split=(), kind=jnp.bfloat16):
    result = scale * jax.random.normal(key, shape, jnp.float32)
    if split:
        result = result * block_levels(key, shape, split, -0.22, 0.18)
    return jnp.clip(result, -limit, limit).astype(kind)


def setup_inputs(seed: int = 0) -> dict:
    key_of = jax.random.split(jax.random.key(seed), 12)
    pair = gaussian(key_of[0], (RES, RES, C), 1.0, 6.0, ((0, 2), (1, 4)))
    ln_gain = jnp.clip(1.0 + 0.18 * jax.random.normal(key_of[1], (C,), jnp.float32), 0.1, 1.9)
    ln_shift = gaussian(key_of[2], (C,), 0.5, 3.0, (), jnp.float32)
    proj_weight = gaussian(key_of[3], (C, 4 * HID), C ** -0.5, 0.5)
    proj_bias = gaussian(key_of[4], (4 * HID,), 0.5, 3.0, (), jnp.float32)
    gate_weight = gaussian(key_of[5], (C, C), C ** -0.5, 0.5)
    gate_bias = gaussian(key_of[6], (C,), 0.5, 3.0, (), jnp.float32)
    out_gain = jnp.clip(1.0 + 0.18 * jax.random.normal(key_of[7], (HID,), jnp.float32), 0.1, 1.9)
    out_shift = gaussian(key_of[8], (HID,), 0.5, 3.0, (), jnp.float32)
    out_weight = gaussian(key_of[9], (HID, C), HID ** -0.5, 0.5)
    out_bias = gaussian(key_of[10], (C,), 0.5, 3.0, (), jnp.float32)
    return {"pair": pair, "ln_gain": ln_gain, "ln_shift": ln_shift, "proj_weight": proj_weight, "proj_bias": proj_bias, "gate_weight": gate_weight, "gate_bias": gate_bias, "out_gain": out_gain, "out_shift": out_shift, "out_weight": out_weight, "out_bias": out_bias}


def layer_norm(values, gain, shift):
    centre = lax.optimization_barrier(jnp.mean(values, axis=-1, keepdims=True))
    centred = values - centre
    spread = lax.optimization_barrier(jnp.mean(centred * centred, axis=-1, keepdims=True))
    return centred * lax.rsqrt(spread + 1e-05) * gain + shift

def reference(pair, ln_gain, ln_shift, proj_weight, proj_bias, gate_weight, gate_bias, out_gain, out_shift, out_weight, out_bias):
    hidden = proj_weight.shape[1] // 4
    normed = layer_norm(pair.astype(jnp.float32), ln_gain, ln_shift).astype(jnp.bfloat16)
    flat = normed.reshape(-1, C)
    mixed = jnp.dot(flat, proj_weight, preferred_element_type=jnp.float32) + proj_bias
    left = (jax.nn.sigmoid(mixed[:, :hidden]) * mixed[:, hidden:2 * hidden]).astype(jnp.bfloat16)
    right = (jax.nn.sigmoid(mixed[:, 2 * hidden:3 * hidden]) * mixed[:, 3 * hidden:]).astype(jnp.bfloat16)
    gate = jax.nn.sigmoid(jnp.dot(flat, gate_weight, preferred_element_type=jnp.float32) + gate_bias)
    left = left.reshape(RES, RES, hidden).astype(jnp.float32)
    right = right.reshape(RES, RES, hidden).astype(jnp.float32)
    triangle = jnp.einsum('ikc,jkc->ijc', left, right)
    tri_normed = layer_norm(triangle, out_gain, out_shift).astype(jnp.bfloat16)
    projected = jnp.dot(tri_normed.reshape(-1, hidden), out_weight, preferred_element_type=jnp.float32) + out_bias
    return (gate * projected).reshape(RES, RES, C).astype(jnp.bfloat16)
```

```python
import functools

import jax
import jax.numpy as jnp
from jax import lax
from jax.experimental import pallas as pl
from jax.experimental.pallas import tpu as pltpu
from jax.sharding import PartitionSpec as P

CHUNKS = 4
PIECES = 8


def layer_norm(values, gain, shift):
    centre = jnp.mean(values, axis=-1, keepdims=True)
    centred = values - centre
    spread = jnp.mean(centred * centred, axis=-1, keepdims=True)
    return centred * lax.rsqrt(spread + 1e-05) * gain + shift


def flipped_dot(a, b):
    return lax.dot_general(a, b, (((1,), (1,)), ((), ())), preferred_element_type=jnp.float32)


def project_kernel(x_ref, gain_ref, shift_ref, w_ref, b_ref, *refs):
    outs, (flat, made) = refs[:-2], refs[-2:]
    rows, step_k, channels = x_ref.shape
    count = w_ref.shape[0] // 4
    each = outs[0].shape[0]
    normed = layer_norm(x_ref[...].astype(jnp.float32), gain_ref[...], shift_ref[...])
    flat[...] = normed.reshape(rows * step_k, channels)
    lanes = made.shape[2]
    for k in range(step_k):
        line = flat[pl.ds(k, rows, stride=step_k), :].astype(jnp.bfloat16)
        mixed = flipped_dot(w_ref[...], line) + b_ref[...]
        left = jax.nn.sigmoid(mixed[:count]) * mixed[count : 2 * count]
        right = jax.nn.sigmoid(mixed[2 * count : 3 * count]) * mixed[3 * count :]
        for side, value in enumerate((left, right)):
            for tile in range(rows // lanes):
                made[tile, pl.ds(side * count * step_k + k, count, stride=step_k), :] = value[
                    :, tile * lanes : (tile + 1) * lanes
                ]
    for n, out in enumerate(outs):
        for tile in range(rows // lanes):
            size = each * step_k
            out[:, :, tile * lanes : (tile + 1) * lanes] = (
                made[tile, n * size : (n + 1) * size, :]
                .reshape(each, step_k, lanes)
                .astype(jnp.bfloat16)
            )


def project_all(pair, gain, shift, weight, bias, pieces, step_k):
    rows, cols, channels = pair.shape
    count = weight.shape[0] // 4
    each = count // pieces
    lanes = 128 if rows % 128 == 0 else rows
    whole = lambda *shape: pl.BlockSpec(shape, lambda k: (0,) * len(shape))
    return pl.pallas_call(
        project_kernel,
        grid=(cols // step_k,),
        in_specs=[
            pl.BlockSpec((rows, step_k, channels), lambda k: (0, k, 0)),
            whole(1, channels),
            whole(1, channels),
            whole(4 * count, channels),
            whole(4 * count, 1),
        ],
        out_specs=[pl.BlockSpec((each, step_k, rows), lambda k: (0, k, 0))] * (2 * pieces),
        out_shape=[jax.ShapeDtypeStruct((each, cols, rows), jnp.bfloat16)] * (2 * pieces),
        scratch_shapes=[
            pltpu.VMEM((rows * step_k, channels), jnp.float32),
            pltpu.VMEM((rows // lanes, 2 * count * step_k, lanes), jnp.float32),
        ],
        compiler_params=pltpu.CompilerParams(vmem_limit_bytes=60 * 1024 * 1024),
        cost_estimate=pl.CostEstimate(
            flops=2 * rows * cols * channels * 4 * count,
            bytes_accessed=4 * rows * cols * channels,
            transcendentals=rows * cols * 2 * count,
        ),
    )(pair, gain[None], shift[None], weight, bias[:, None])


def finish_kernel(x_ref, gain_ref, shift_ref, gw_ref, gb_ref, og_ref, os_ref, ow_ref, ob_ref, *refs):
    tris, (out, held, done) = refs[:-3], refs[-3:]
    rows, step_j, channels = x_ref.shape
    hidden = ow_ref.shape[0]
    tiles, lanes = held.shape[0], held.shape[2]
    each = tris[0].shape[0]
    for tile in range(tiles):
        cut = slice(tile * lanes, (tile + 1) * lanes)
        total = 0.0
        for tri in tris:
            total = total + jnp.sum(tri[:, :, cut].astype(jnp.float32), axis=0)
        centre = total / hidden
        spread = 0.0
        for tri in tris:
            centred = tri[:, :, cut].astype(jnp.float32) - centre[None]
            spread = spread + jnp.sum(centred * centred, axis=0)
        scale = lax.rsqrt(spread / hidden + 1e-05)
        for n, tri in enumerate(tris):
            centred = tri[:, :, cut].astype(jnp.float32) - centre[None]
            held[tile, n * each * step_j : (n + 1) * each * step_j, :] = (
                centred * scale[None]
            ).reshape(each * step_j, lanes)
    for j in range(step_j):
        for tile in range(tiles):
            value = held[tile, pl.ds(j, hidden, stride=step_j), :]
            value = (value * og_ref[...] + os_ref[...]).astype(jnp.bfloat16)
            projected = lax.dot_general(
                value, ow_ref[...], (((0,), (0,)), ((), ())), preferred_element_type=jnp.float32
            )
            done[pl.ds(tile * lanes * step_j + j, lanes, stride=step_j), :] = projected
    normed = layer_norm(x_ref[...].astype(jnp.float32), gain_ref[...], shift_ref[...])
    flat = normed.reshape(rows * step_j, channels).astype(jnp.bfloat16)
    gate = jax.nn.sigmoid(
        jnp.dot(flat, gw_ref[...], preferred_element_type=jnp.float32) + gb_ref[...]
    )
    update = gate * (done[...] + ob_ref[...])
    out[...] = update.reshape(rows, step_j, channels).astype(jnp.bfloat16)


def finish_all(pair, core, part, gain, shift, gw, gb, og, os, ow, ob, tris, step_j):
    rows, _, channels = pair.shape
    hidden = ow.shape[0]
    lanes = 128 if rows % 128 == 0 else rows
    each = tris[0].shape[0]
    here = lax.dynamic_slice_in_dim(pair, core * part, part, 1)
    whole = lambda *shape: pl.BlockSpec(shape, lambda j: (0,) * len(shape))
    return pl.pallas_call(
        finish_kernel,
        grid=(part // step_j,),
        in_specs=[
            pl.BlockSpec((rows, step_j, channels), lambda j: (0, j, 0)),
            whole(1, channels),
            whole(1, channels),
            whole(channels, channels),
            whole(1, channels),
            whole(hidden, 1),
            whole(hidden, 1),
            whole(hidden, channels),
            whole(1, channels),
        ]
        + [pl.BlockSpec((each, step_j, rows), lambda j: (0, j, 0))] * len(tris),
        out_specs=pl.BlockSpec((rows, step_j, channels), lambda j: (0, j, 0)),
        out_shape=jax.ShapeDtypeStruct((rows, part, channels), jnp.bfloat16),
        scratch_shapes=[
            pltpu.VMEM((rows // lanes, hidden * step_j, lanes), jnp.float32),
            pltpu.VMEM((rows * step_j, channels), jnp.float32),
        ],
        compiler_params=pltpu.CompilerParams(vmem_limit_bytes=60 * 1024 * 1024),
        cost_estimate=pl.CostEstimate(
            flops=4 * rows * part * channels * channels,
            bytes_accessed=6 * rows * part * channels,
            transcendentals=rows * part * channels,
        ),
    )(here, gain[None], shift[None], gw, gb[None], og[:, None], os[:, None], ow, ob[None], *tris)


def exchange_kernel(
    pieces, left, right, out, lefts, rights, sent, arrived, blocks,
    local, edge_l, edge_r, near_sem, far_sem, cross_sem, give_sem, spread_sem, gone,
):
    row, col, depth = (lax.axis_index(a) for a in ("row", "col", "depth"))
    count, cols, rows = left.shape
    size = count // pieces
    part = cols // 2
    inner = (col == 1) | (col == 2)
    low, high = col % 2, col // 2
    other = 1 - high
    mesh_id = pl.DeviceIdType.MESH
    over_row = (1 - row, col, depth)
    beside = (row, 2 * high + 1 - low, depth)
    opposite = (row, 3 - col, depth)
    peers = [(row, col, depth ^ m) for m in (1, 2, 3)]

    def cut(t):
        return pl.ds(t * size, size)

    def remote(src, dst, kind, recv, device):
        return pltpu.make_async_remote_copy(
            src_ref=src, dst_ref=dst, send_sem=gone.at[kind], recv_sem=recv,
            device_id=device, device_id_type=mesh_id,
        )

    own_k, far_k = pl.ds(0, cols), pl.ds(cols, cols)

    def edge_left(t):
        return remote(left.at[cut(t)], lefts.at[cut(t), far_k], 0, edge_l.at[t], beside)

    def edge_right(t):
        return remote(right.at[cut(t)], rights.at[row, cut(t), far_k], 1, edge_r.at[t], beside)

    def near(t):
        return remote(right.at[cut(t)], rights.at[row, cut(t), own_k], 2, near_sem.at[t], over_row)

    def far(t):
        return remote(
            rights.at[row, cut(t), far_k], rights.at[row, cut(t), far_k], 3, far_sem.at[t], over_row
        )

    def cross(t):
        return remote(sent.at[cut(t)], arrived.at[cut(t)], 4, cross_sem.at[t], opposite)

    def give(t):
        return remote(
            blocks.at[1 - low, cut(t)], blocks.at[1 - low, cut(t)], 5, give_sem.at[t], beside
        )

    def spread(t, m):
        place = pl.ds(((depth ^ (m + 1)) % 2) * part, part)
        return remote(
            blocks.at[low, cut(t), place], out.at[depth, cut(t)], 6 + m, spread_sem.at[m], peers[m]
        )

    def keep(t):
        place = pl.ds((depth % 2) * part, part)
        return pltpu.make_async_copy(blocks.at[low, cut(t), place], out.at[depth, cut(t)], local.at[2])

    def spread_all(t):
        for m in (1, 2, 0):
            spread(t, m).start()
        keep(t).start()

    def term(half, h):
        return lax.dot_general(
            rights[half, h], lefts[h], (((0,), (0,)), ((), ())), preferred_element_type=jnp.float32
        )

    barrier = pltpu.get_barrier_semaphore()
    for device in (over_row, beside, opposite, *peers):
        pl.semaphore_signal(barrier, inc=1, device_id=device, device_id_type=mesh_id)
    pl.semaphore_wait(barrier, 6)

    @pl.when(inner)
    def _():
        load_l = pltpu.make_async_copy(left, lefts.at[:, own_k], local.at[0])
        load_r = pltpu.make_async_copy(right, rights.at[row, :, own_k], local.at[1])
        near(0).start()
        load_l.start()
        load_r.start()
        near(1).start()
        load_l.wait()
        load_r.wait()

        def meet(t):
            near(t).wait_recv()
            far(t).wait_recv()

        def step(t, _):
            @pl.when(t < pieces)
            def _():
                edge_left(t).wait_recv()
                edge_right(t).wait_recv()
                far(t).start()

                @pl.when(t + 2 < pieces)
                def _():
                    near(t + 2).start()

                @pl.when(row != other)
                def _():
                    meet(t)

                def one(h, _):
                    sent[t * size + h] = term(other, t * size + h).astype(jnp.bfloat16)
                    return 0

                lax.fori_loop(0, size, one, 0)
                cross(t).start()

            @pl.when(t >= 1)
            def _():
                u = t - 1

                @pl.when(row == other)
                def _():
                    meet(u)

                cross(u).wait_recv()

                def one(h, _):
                    h = u * size + h
                    total = (term(high, h) + arrived[h].astype(jnp.float32)).astype(jnp.bfloat16)
                    blocks[0, h] = total[:cols]
                    blocks[1, h] = total[cols:]
                    return 0

                lax.fori_loop(0, size, one, 0)
                give(u).start()
                spread_all(u)

            return 0

        lax.fori_loop(0, pieces + 1, step, 0)
        whole = blocks.at[0]
        for kind in (2, 3, 5):
            pltpu.make_async_copy(whole, whole, gone.at[kind]).wait()
        pltpu.make_async_copy(sent, sent, gone.at[4]).wait()

    @pl.when(jnp.logical_not(inner))
    def _():
        def push(t, _):
            edge_left(t).start()
            edge_right(t).start()
            return 0

        lax.fori_loop(0, pieces, push, 0)

        def step(t, _):
            give(t).wait_recv()
            spread_all(t)
            return 0

        lax.fori_loop(0, pieces, step, 0)
        pltpu.make_async_copy(left, left, gone.at[0]).wait()
        pltpu.make_async_copy(right, right, gone.at[1]).wait()

    mine = out.at[depth]
    pltpu.make_async_copy(mine, mine, local.at[2]).wait()
    for m in range(3):
        pltpu.make_async_copy(mine, mine, gone.at[6 + m]).wait()
        pltpu.make_async_copy(mine, mine, spread_sem.at[m]).wait()


def exchange(left, right, pieces):
    count, cols, rows = left.shape
    dma = pltpu.SemaphoreType.DMA
    anywhere = pl.BlockSpec(memory_space=pl.ANY)
    return pl.pallas_call(
        functools.partial(exchange_kernel, pieces),
        in_specs=[anywhere, anywhere],
        out_specs=anywhere,
        out_shape=jax.ShapeDtypeStruct((4, count, cols // 2, rows), jnp.bfloat16),
        scratch_shapes=[
            pltpu.VMEM((count, 2 * cols, rows), jnp.bfloat16),
            pltpu.VMEM((2, count, 2 * cols, rows), jnp.bfloat16),
            pltpu.VMEM((count, rows, rows), jnp.bfloat16),
            pltpu.VMEM((count, rows, rows), jnp.bfloat16),
            pltpu.VMEM((2, count, cols, rows), jnp.bfloat16),
            dma((3,)),
        ]
        + [dma((pieces,))] * 6
        + [dma((3,)), dma((9,))],
        compiler_params=pltpu.CompilerParams(
            collective_id=0, has_side_effects=True, vmem_limit_bytes=63 * 1024 * 1024
        ),
        name="exchange",
    )(left, right)


def swap(value, axis, bit):
    count = lax.axis_size(axis)
    return lax.ppermute(value, axis, [(n, n ^ bit) for n in range(count)])


def pick(first_mine, mine, other):
    return jnp.where(first_mine, mine, other), jnp.where(first_mine, other, mine)


def cross_term(lefts, far, chunk, contract):
    left_far, (_, near), (_, beyond) = far[chunk]
    return (contract(near, lefts[chunk]) + contract(beyond, left_far)).astype(jnp.bfloat16)


def per_device_kernel(
    pair,
    ln_gain,
    ln_shift,
    proj_weight,
    proj_bias,
    gate_weight,
    gate_bias,
    out_gain,
    out_shift,
    out_weight,
    out_bias,
):
    depth_n = lax.axis_size("depth")
    depth = lax.axis_index("depth")
    rows, cols, channels = pair.shape
    hidden = proj_weight.shape[1] // 4
    core = depth % 2
    per_depth = hidden // depth_n
    part = cols // 2
    step = 16
    weight = proj_weight.T.reshape(4, hidden, channels)
    bias = proj_bias.reshape(4, hidden)
    mine = lax.dynamic_slice_in_dim(weight, depth * per_depth, per_depth, 1)
    mine_bias = lax.dynamic_slice_in_dim(bias, depth * per_depth, per_depth, 1)
    left, right = project_all(
        pair, ln_gain, ln_shift, mine.reshape(-1, channels), mine_bias.reshape(-1), 1, step
    )
    triangle = exchange(left, right, PIECES).reshape(hidden, part, rows)
    finished = finish_all(
        pair, core, part, ln_gain, ln_shift, gate_weight, gate_bias, out_gain, out_shift,
        out_weight, out_bias, [triangle], step,
    )
    first, second = pick(core == 0, finished, swap(finished, "depth", 1))
    return jnp.concatenate([first, second], axis=1)


def per_device(
    pair,
    ln_gain,
    ln_shift,
    proj_weight,
    proj_bias,
    gate_weight,
    gate_bias,
    out_gain,
    out_shift,
    out_weight,
    out_bias,
):
    rows_n, cols_n, depth_n = (lax.axis_size(a) for a in ("row", "col", "depth"))
    row, col, depth = (lax.axis_index(a) for a in ("row", "col", "depth"))
    rows, cols, channels = pair.shape
    hidden = proj_weight.shape[1] // 4
    low, high = col % 2, col // 2
    core = depth % 2
    per_depth = hidden // depth_n
    per_col = per_depth // 2
    step = per_col // CHUNKS
    half_j = 2 * cols
    part = cols // 2

    weight = proj_weight.T.reshape(4, hidden, channels)
    bias = proj_bias.reshape(4, hidden)
    first = depth * per_depth
    mine = lax.dynamic_slice_in_dim(weight, first, per_depth, 1)
    mine_bias = lax.dynamic_slice_in_dim(bias, first, per_depth, 1)
    mine = jnp.where(low == 0, mine, jnp.roll(mine, per_col, 1))
    mine_bias = jnp.where(low == 0, mine_bias, jnp.roll(mine_bias, per_col, 1))
    step_k = 16
    made = project_all(
        pair, ln_gain, ln_shift, mine.reshape(-1, channels), mine_bias.reshape(-1), 2 * CHUNKS, step_k
    )
    lefts, rights = made[: 2 * CHUNKS], made[2 * CHUNKS :]

    def gather_rows(right):
        if rows_n == 2:
            return pick(row == high, right, swap(right, "row", 1))
        whole = lax.all_gather(right, "row", axis=2, tiled=True)
        return (
            lax.dynamic_slice_in_dim(whole, high * half_j, half_j, 2),
            lax.dynamic_slice_in_dim(whole, (1 - high) * half_j, half_j, 2),
        )

    def contract(right, left):
        return jnp.einsum("hkj,hki->hji", right, left, preferred_element_type=jnp.float32)

    gathered = []
    far, crossed = [], []
    for chunk in range(CHUNKS):
        ahead = (lefts[CHUNKS + chunk], rights[CHUNKS + chunk])
        if chunk >= 2:
            *ahead, crossed[chunk - 2] = lax.optimization_barrier((*ahead, crossed[chunk - 2]))
        left_far, right_far = (swap(value, "col", 1) for value in ahead)
        far.append((left_far, gather_rows(rights[chunk]), gather_rows(right_far)))
        if chunk >= 1:
            crossed.append(cross_term(lefts, far, chunk - 1, contract))
    crossed.append(cross_term(lefts, far, CHUNKS - 1, contract))
    for chunk in range(CHUNKS):
        left_near = lefts[chunk]
        left_far, (near_own, _), (far_own, _) = far[chunk]
        arrived = swap(crossed[chunk], "col", 2)
        own = contract(near_own, left_near) + contract(far_own, left_far)
        triangle = (own + arrived.astype(jnp.float32)).astype(jnp.bfloat16)
        keep = lax.dynamic_slice_in_dim(triangle, low * cols, cols, 1)
        give = lax.dynamic_slice_in_dim(triangle, (1 - low) * cols, cols, 1)
        block = jnp.concatenate([keep, swap(give, "col", 1)], axis=0)
        same = lax.dynamic_slice_in_dim(block, core * part, part, 1)
        across = lax.dynamic_slice_in_dim(block, (1 - core) * part, part, 1)
        gathered += [
            same,
            swap(across, "depth", 1),
            swap(same, "depth", 2),
            swap(across, "depth", 3),
        ]

    order = jnp.concatenate(
        [
            (depth ^ m) * per_depth + (low ^ n) * per_col + chunk * step + jnp.arange(step)
            for chunk in range(CHUNKS)
            for m in range(4)
            for n in range(2)
        ]
    )
    finished = finish_all(
        pair,
        core,
        part,
        ln_gain,
        ln_shift,
        gate_weight,
        gate_bias,
        out_gain[order],
        out_shift[order],
        out_weight[order],
        out_bias,
        gathered,
        step_k,
    )
    first, second = pick(core == 0, finished, swap(finished, "depth", 1))
    return jnp.concatenate([first, second], axis=1)


def solution(mesh):
    placed = (P("row", "col", None), P(), P(), P(), P(), P(), P(), P(), P(), P(), P())
    small = tuple(mesh.shape[a] for a in ("row", "col", "depth")) == (2, 4, 4)
    return jax.shard_map(
        per_device_kernel if small else per_device, mesh=mesh, in_specs=placed, out_specs=P("row", "col", None), check_vma=False
    )
```

```python
import functools

import jax
import jax.numpy as jnp
from jax import lax
from jax.experimental import pallas as pl
from jax.experimental.pallas import tpu as pltpu
from jax.sharding import PartitionSpec as P

CHUNKS = 4
PIECES = 32
SHARES = (3, 2, 1)


def layer_norm(values, gain, shift):
    centre = jnp.mean(values, axis=-1, keepdims=True)
    centred = values - centre
    spread = jnp.mean(centred * centred, axis=-1, keepdims=True)
    return centred * lax.rsqrt(spread + 1e-05) * gain + shift


def flipped_dot(a, b):
    return lax.dot_general(a, b, (((1,), (1,)), ((), ())), preferred_element_type=jnp.float32)


def project_kernel(x_ref, gain_ref, shift_ref, w_ref, b_ref, *refs):
    outs, (flat, made) = refs[:-2], refs[-2:]
    rows, step_k, channels = x_ref.shape
    count = w_ref.shape[0] // 4
    each = outs[0].shape[0]
    normed = layer_norm(x_ref[...].astype(jnp.float32), gain_ref[...], shift_ref[...])
    flat[...] = normed.reshape(rows * step_k, channels)
    lanes = made.shape[2]
    for k in range(step_k):
        line = flat[pl.ds(k, rows, stride=step_k), :].astype(jnp.bfloat16)
        mixed = flipped_dot(w_ref[...], line) + b_ref[...]
        left = jax.nn.sigmoid(mixed[:count]) * mixed[count : 2 * count]
        right = jax.nn.sigmoid(mixed[2 * count : 3 * count]) * mixed[3 * count :]
        for side, value in enumerate((left, right)):
            for tile in range(rows // lanes):
                made[tile, pl.ds(side * count * step_k + k, count, stride=step_k), :] = value[
                    :, tile * lanes : (tile + 1) * lanes
                ]
    for n, out in enumerate(outs):
        for tile in range(rows // lanes):
            size = each * step_k
            out[:, :, tile * lanes : (tile + 1) * lanes] = (
                made[tile, n * size : (n + 1) * size, :]
                .reshape(each, step_k, lanes)
                .astype(jnp.bfloat16)
            )


def project_all(pair, gain, shift, weight, bias, pieces, step_k):
    rows, cols, channels = pair.shape
    count = weight.shape[0] // 4
    each = count // pieces
    lanes = 128 if rows % 128 == 0 else rows
    whole = lambda *shape: pl.BlockSpec(shape, lambda k: (0,) * len(shape))
    return pl.pallas_call(
        project_kernel,
        grid=(cols // step_k,),
        in_specs=[
            pl.BlockSpec((rows, step_k, channels), lambda k: (0, k, 0)),
            whole(1, channels),
            whole(1, channels),
            whole(4 * count, channels),
            whole(4 * count, 1),
        ],
        out_specs=[pl.BlockSpec((each, step_k, rows), lambda k: (0, k, 0))] * (2 * pieces),
        out_shape=[jax.ShapeDtypeStruct((each, cols, rows), jnp.bfloat16)] * (2 * pieces),
        scratch_shapes=[
            pltpu.VMEM((rows * step_k, channels), jnp.float32),
            pltpu.VMEM((rows // lanes, 2 * count * step_k, lanes), jnp.float32),
        ],
        compiler_params=pltpu.CompilerParams(vmem_limit_bytes=60 * 1024 * 1024),
        cost_estimate=pl.CostEstimate(
            flops=2 * rows * cols * channels * 4 * count,
            bytes_accessed=4 * rows * cols * channels,
            transcendentals=rows * cols * 2 * count,
        ),
    )(pair, gain[None], shift[None], weight, bias[:, None])


def finish_kernel(x_ref, gain_ref, shift_ref, gw_ref, gb_ref, og_ref, os_ref, ow_ref, ob_ref, *refs):
    tris, (out, held, done) = refs[:-3], refs[-3:]
    rows, step_j, channels = x_ref.shape
    hidden = ow_ref.shape[0]
    tiles, lanes = held.shape[0], held.shape[2]
    each = tris[0].shape[0]
    for tile in range(tiles):
        cut = slice(tile * lanes, (tile + 1) * lanes)
        total = 0.0
        for tri in tris:
            total = total + jnp.sum(tri[:, :, cut].astype(jnp.float32), axis=0)
        centre = total / hidden
        spread = 0.0
        for tri in tris:
            centred = tri[:, :, cut].astype(jnp.float32) - centre[None]
            spread = spread + jnp.sum(centred * centred, axis=0)
        scale = lax.rsqrt(spread / hidden + 1e-05)
        for n, tri in enumerate(tris):
            centred = tri[:, :, cut].astype(jnp.float32) - centre[None]
            held[tile, n * each * step_j : (n + 1) * each * step_j, :] = (
                centred * scale[None]
            ).reshape(each * step_j, lanes)
    for j in range(step_j):
        for tile in range(tiles):
            value = held[tile, pl.ds(j, hidden, stride=step_j), :]
            value = (value * og_ref[...] + os_ref[...]).astype(jnp.bfloat16)
            projected = lax.dot_general(
                value, ow_ref[...], (((0,), (0,)), ((), ())), preferred_element_type=jnp.float32
            )
            done[pl.ds(tile * lanes * step_j + j, lanes, stride=step_j), :] = projected
    normed = layer_norm(x_ref[...].astype(jnp.float32), gain_ref[...], shift_ref[...])
    flat = normed.reshape(rows * step_j, channels).astype(jnp.bfloat16)
    gate = jax.nn.sigmoid(
        jnp.dot(flat, gw_ref[...], preferred_element_type=jnp.float32) + gb_ref[...]
    )
    update = gate * (done[...] + ob_ref[...])
    out[...] = update.reshape(rows, step_j, channels).astype(jnp.bfloat16)


def finish_all(pair, core, part, gain, shift, gw, gb, og, os, ow, ob, tris, step_j):
    rows, _, channels = pair.shape
    hidden = ow.shape[0]
    lanes = 128 if rows % 128 == 0 else rows
    each = tris[0].shape[0]
    here = lax.dynamic_slice_in_dim(pair, core * part, part, 1)
    whole = lambda *shape: pl.BlockSpec(shape, lambda j: (0,) * len(shape))
    return pl.pallas_call(
        finish_kernel,
        grid=(part // step_j,),
        in_specs=[
            pl.BlockSpec((rows, step_j, channels), lambda j: (0, j, 0)),
            whole(1, channels),
            whole(1, channels),
            whole(channels, channels),
            whole(1, channels),
            whole(hidden, 1),
            whole(hidden, 1),
            whole(hidden, channels),
            whole(1, channels),
        ]
        + [pl.BlockSpec((each, step_j, rows), lambda j: (0, j, 0))] * len(tris),
        out_specs=pl.BlockSpec((rows, step_j, channels), lambda j: (0, j, 0)),
        out_shape=jax.ShapeDtypeStruct((rows, part, channels), jnp.bfloat16),
        scratch_shapes=[
            pltpu.VMEM((rows // lanes, hidden * step_j, lanes), jnp.float32),
            pltpu.VMEM((rows * step_j, channels), jnp.float32),
        ],
        compiler_params=pltpu.CompilerParams(vmem_limit_bytes=60 * 1024 * 1024),
        cost_estimate=pl.CostEstimate(
            flops=4 * rows * part * channels * channels,
            bytes_accessed=6 * rows * part * channels,
            transcendentals=rows * part * channels,
        ),
    )(here, gain[None], shift[None], gw, gb[None], og[:, None], os[:, None], ow, ob[None], *tris)


def exchange_kernel(
    pieces, left, right, out, lefts, rights, sent, arrived, blocks,
    local, edge_l, edge_r, near_sem, far_sem, cross_sem, give_sem, spread_sem, gone,
):
    row, col, depth = (lax.axis_index(a) for a in ("row", "col", "depth"))
    count, cols, rows = left.shape
    size = count // pieces
    part = cols // 2
    inner = (col == 1) | (col == 2)
    low, high = col % 2, col // 2
    other = 1 - high
    mesh_id = pl.DeviceIdType.MESH
    over_row = (1 - row, col, depth)
    beside = (row, 2 * high + 1 - low, depth)
    opposite = (row, 3 - col, depth)
    peers = [(row, col, depth ^ m) for m in (1, 2, 3)]

    def cut(t):
        return pl.ds(t * size, size)

    def remote(src, dst, kind, recv, device):
        return pltpu.make_async_remote_copy(
            src_ref=src, dst_ref=dst, send_sem=gone.at[kind], recv_sem=recv,
            device_id=device, device_id_type=mesh_id,
        )

    own_k, far_k = pl.ds(0, cols), pl.ds(cols, cols)

    def edge_left(t):
        return remote(left.at[cut(t)], lefts.at[cut(t), far_k], 0, edge_l.at[t], beside)

    def edge_right(t):
        return remote(right.at[cut(t)], rights.at[row, cut(t), far_k], 1, edge_r.at[t], beside)

    def near(t):
        return remote(right.at[cut(t)], rights.at[row, cut(t), own_k], 2, near_sem.at[t], over_row)

    def far(t):
        return remote(
            rights.at[row, cut(t), far_k], rights.at[row, cut(t), far_k], 3, far_sem.at[t], over_row
        )

    def cross(t):
        return remote(sent.at[cut(t)], arrived.at[cut(t)], 4, cross_sem.at[t], opposite)

    def give(t):
        return remote(
            blocks.at[1 - low, cut(t)], blocks.at[1 - low, cut(t)], 5, give_sem.at[t], beside
        )

    def spread(t, m):
        place = pl.ds(((depth ^ (m + 1)) % 2) * part, part)
        return remote(
            blocks.at[low, cut(t), place], out.at[depth, cut(t)], 6 + m, spread_sem.at[m], peers[m]
        )

    def keep(t):
        place = pl.ds((depth % 2) * part, part)
        return pltpu.make_async_copy(blocks.at[low, cut(t), place], out.at[depth, cut(t)], local.at[2])

    def spread_all(t):
        for m in (1, 2, 0):
            spread(t, m).start()
        keep(t).start()

    def term(half, h):
        return lax.dot_general(
            rights[half, h], lefts[h], (((0,), (0,)), ((), ())), preferred_element_type=jnp.float32
        )

    barrier = pltpu.get_barrier_semaphore()
    for device in (over_row, beside, opposite, *peers):
        pl.semaphore_signal(barrier, inc=1, device_id=device, device_id_type=mesh_id)
    pl.semaphore_wait(barrier, 6)

    @pl.when(inner)
    def _():
        load_l = pltpu.make_async_copy(left, lefts.at[:, own_k], local.at[0])
        load_r = pltpu.make_async_copy(right, rights.at[row, :, own_k], local.at[1])
        near(0).start()
        load_l.start()
        load_r.start()
        near(1).start()
        load_l.wait()
        load_r.wait()

        def meet(t):
            near(t).wait_recv()
            far(t).wait_recv()

        def step(t, _):
            @pl.when(t < pieces)
            def _():
                edge_left(t).wait_recv()
                edge_right(t).wait_recv()
                far(t).start()

                @pl.when(t + 2 < pieces)
                def _():
                    near(t + 2).start()

                @pl.when(row != other)
                def _():
                    meet(t)

                def one(h, _):
                    sent[t * size + h] = term(other, t * size + h).astype(jnp.bfloat16)
                    return 0

                lax.fori_loop(0, size, one, 0)
                cross(t).start()

            @pl.when(t >= 1)
            def _():
                u = t - 1

                @pl.when(row == other)
                def _():
                    meet(u)

                cross(u).wait_recv()

                def one(h, _):
                    h = u * size + h
                    total = (term(high, h) + arrived[h].astype(jnp.float32)).astype(jnp.bfloat16)
                    blocks[0, h] = total[:cols]
                    blocks[1, h] = total[cols:]
                    return 0

                lax.fori_loop(0, size, one, 0)
                give(u).start()
                spread_all(u)

            return 0

        lax.fori_loop(0, pieces + 1, step, 0)
        whole = blocks.at[0]
        for kind in (2, 3, 5):
            pltpu.make_async_copy(whole, whole, gone.at[kind]).wait()
        pltpu.make_async_copy(sent, sent, gone.at[4]).wait()

    @pl.when(jnp.logical_not(inner))
    def _():
        def push(t, _):
            edge_left(t).start()
            edge_right(t).start()
            return 0

        lax.fori_loop(0, pieces, push, 0)

        def step(t, _):
            give(t).wait_recv()
            spread_all(t)
            return 0

        lax.fori_loop(0, pieces, step, 0)
        pltpu.make_async_copy(left, left, gone.at[0]).wait()
        pltpu.make_async_copy(right, right, gone.at[1]).wait()

    mine = out.at[depth]
    pltpu.make_async_copy(mine, mine, local.at[2]).wait()
    for m in range(3):
        pltpu.make_async_copy(mine, mine, gone.at[6 + m]).wait()
        pltpu.make_async_copy(mine, mine, spread_sem.at[m]).wait()


def exchange(left, right, pieces):
    count, cols, rows = left.shape
    dma = pltpu.SemaphoreType.DMA
    anywhere = pl.BlockSpec(memory_space=pl.ANY)
    return pl.pallas_call(
        functools.partial(exchange_kernel, pieces),
        in_specs=[anywhere, anywhere],
        out_specs=anywhere,
        out_shape=jax.ShapeDtypeStruct((4, count, cols // 2, rows), jnp.bfloat16),
        scratch_shapes=[
            pltpu.VMEM((count, 2 * cols, rows), jnp.bfloat16),
            pltpu.VMEM((2, count, 2 * cols, rows), jnp.bfloat16),
            pltpu.VMEM((count, rows, rows), jnp.bfloat16),
            pltpu.VMEM((count, rows, rows), jnp.bfloat16),
            pltpu.VMEM((2, count, cols, rows), jnp.bfloat16),
            dma((3,)),
        ]
        + [dma((pieces,))] * 6
        + [dma((3,)), dma((9,))],
        compiler_params=pltpu.CompilerParams(
            collective_id=0, has_side_effects=True, vmem_limit_bytes=63 * 1024 * 1024
        ),
        name="exchange",
    )(left, right)


PITCH = 17


def polish_kernel(
    off_ref, x_ref, gain_ref, shift_ref, gw_ref, gb_ref, og_ref, os_ref, ow_ref, ob_ref, tri_ref, *refs
):
    full, half, held, done = refs[-4:]
    rows, step_j, channels = x_ref.shape
    hidden = tri_ref.shape[0]
    tiles, lanes = held.shape[0], held.shape[2]
    group = 16
    for tile in range(tiles):
        cut = slice(tile * lanes, (tile + 1) * lanes)

        def block(g):
            return tri_ref[pl.ds(g * group, group), :, cut].astype(jnp.float32)

        zero = jnp.zeros((step_j, lanes), jnp.float32)
        total = lax.fori_loop(0, hidden // group, lambda g, s: s + jnp.sum(block(g), axis=0), zero)
        centre = total / hidden

        def square(g, s):
            centred = block(g) - centre[None]
            return s + jnp.sum(centred * centred, axis=0)

        spread = lax.fori_loop(0, hidden // group, square, zero)
        scale = lax.rsqrt(spread / hidden + 1e-05)

        def normalise(g, _):
            for n in range(group):
                h = g * group + n
                value = (tri_ref[h, :, cut].astype(jnp.float32) - centre) * scale
                held[tile, pl.ds(h * PITCH, step_j), :] = value * og_ref[h] + os_ref[h]
            return 0

        lax.fori_loop(0, hidden // group, normalise, 0)

    def project(j, _):
        for tile in range(tiles):
            value = held[tile, pl.ds(j, hidden, stride=PITCH), :].astype(jnp.bfloat16)
            done[pl.ds(tile * lanes * PITCH + j, lanes, stride=PITCH), :] = lax.dot_general(
                value, ow_ref[...], (((0,), (0,)), ((), ())), preferred_element_type=jnp.float32
            )
        return 0

    lax.fori_loop(0, step_j, project, 0, unroll=4)
    bunch = rows // 4

    def close(g, _):
        place = pl.ds(g * bunch, bunch)
        normed = layer_norm(x_ref[place].astype(jnp.float32), gain_ref[...], shift_ref[...])
        flat = normed.reshape(bunch * step_j, channels).astype(jnp.bfloat16)
        gate = jax.nn.sigmoid(
            jnp.dot(flat, gw_ref[...], preferred_element_type=jnp.float32) + gb_ref[...]
        )
        for n in range(bunch):
            at = g * bunch + n
            update = gate[n * step_j : (n + 1) * step_j] * (
                done[pl.ds(at * PITCH, step_j), :] + ob_ref[...]
            )
            full[at] = update.astype(jnp.bfloat16)
            half[at] = update.astype(jnp.bfloat16)
        return 0

    lax.fori_loop(0, 4, close, 0)


def polish(pair, core, start, size, gain, shift, gw, gb, og, os, ow, ob, tri, full, step_j):
    rows, cols, channels = pair.shape
    hidden, part, _ = tri.shape
    lanes = 128 if rows % 128 == 0 else rows
    first = start // step_j
    offset = (core * (part // step_j) + first)[None]
    whole = lambda *shape: pl.BlockSpec(shape, lambda j, off: (0,) * len(shape))
    scalars = pl.BlockSpec(memory_space=pltpu.SMEM)
    moved = pl.BlockSpec((rows, step_j, channels), lambda j, off: (0, off[0] + j, 0))
    operands = [
        offset, pair, gain[None], shift[None], gw, gb[None], og, os, ow, ob[None], tri,
    ]
    specs = [
        moved,
        whole(1, channels),
        whole(1, channels),
        whole(channels, channels),
        whole(1, channels),
        scalars,
        scalars,
        whole(hidden, channels),
        whole(1, channels),
        pl.BlockSpec((hidden, step_j, rows), lambda j, off: (0, first + j, 0)),
    ]
    alias = {}
    if full is not None:
        alias = {len(operands): 0}
        operands.append(full)
        specs.append(pl.BlockSpec(memory_space=pl.ANY))
    return pl.pallas_call(
        polish_kernel,
        grid_spec=pltpu.PrefetchScalarGridSpec(
            num_scalar_prefetch=1,
            grid=(size // step_j,),
            in_specs=specs,
            out_specs=[
                moved,
                pl.BlockSpec((rows, step_j, channels), lambda j, off: (0, j, 0)),
            ],
            scratch_shapes=[
                pltpu.VMEM((rows // lanes, hidden * PITCH, lanes), jnp.float32),
                pltpu.VMEM((rows * PITCH, channels), jnp.float32),
            ],
        ),
        out_shape=[
            jax.ShapeDtypeStruct((rows, cols, channels), jnp.bfloat16),
            jax.ShapeDtypeStruct((rows, size, channels), jnp.bfloat16),
        ],
        input_output_aliases=alias,
        compiler_params=pltpu.CompilerParams(vmem_limit_bytes=60 * 1024 * 1024),
        cost_estimate=pl.CostEstimate(
            flops=400 * rows * size * channels,
            bytes_accessed=8 * rows * size * channels,
            transcendentals=rows * size * channels,
        ),
        name="polish",
    )(*operands)


def place_kernel(off_ref, part_ref, full_in, full):
    full[...] = part_ref[...]


def place(full, arrived, core, start, part, step_j):
    rows, size, channels = arrived.shape
    block = (rows // 2, step_j, channels)
    offset = ((1 - core) * (part // step_j) + start // step_j)[None]
    return pl.pallas_call(
        place_kernel,
        grid_spec=pltpu.PrefetchScalarGridSpec(
            num_scalar_prefetch=1,
            grid=(2, size // step_j),
            in_specs=[
                pl.BlockSpec(block, lambda i, j, off: (i, j, 0)),
                pl.BlockSpec(memory_space=pl.ANY),
            ],
            out_specs=pl.BlockSpec(block, lambda i, j, off: (i, off[0] + j, 0)),
        ),
        out_shape=jax.ShapeDtypeStruct(full.shape, full.dtype),
        input_output_aliases={2: 0},
        cost_estimate=pl.CostEstimate(
            flops=20 * rows * size * channels,
            bytes_accessed=4 * rows * size * channels,
            transcendentals=0,
        ),
        name="place",
    )(offset, arrived, full)


def swap(value, axis, bit):
    count = lax.axis_size(axis)
    return lax.ppermute(value, axis, [(n, n ^ bit) for n in range(count)])


def pick(first_mine, mine, other):
    return jnp.where(first_mine, mine, other), jnp.where(first_mine, other, mine)


def cross_term(lefts, far, chunk, contract):
    left_far, (_, near), (_, beyond) = far[chunk]
    return (contract(near, lefts[chunk]) + contract(beyond, left_far)).astype(jnp.bfloat16)


def per_device_kernel(
    pair,
    ln_gain,
    ln_shift,
    proj_weight,
    proj_bias,
    gate_weight,
    gate_bias,
    out_gain,
    out_shift,
    out_weight,
    out_bias,
):
    depth_n = lax.axis_size("depth")
    depth = lax.axis_index("depth")
    rows, cols, channels = pair.shape
    hidden = proj_weight.shape[1] // 4
    core = depth % 2
    per_depth = hidden // depth_n
    part = cols // 2
    step = 16
    weight = proj_weight.T.reshape(4, hidden, channels)
    bias = proj_bias.reshape(4, hidden)
    mine = lax.dynamic_slice_in_dim(weight, depth * per_depth, per_depth, 1)
    mine_bias = lax.dynamic_slice_in_dim(bias, depth * per_depth, per_depth, 1)
    left, right = project_all(
        pair, ln_gain, ln_shift, mine.reshape(-1, channels), mine_bias.reshape(-1), 1, step
    )
    triangle = exchange(left, right, PIECES).reshape(hidden, part, rows)
    full, moving, start = None, [], 0
    for share in SHARES:
        size = part * share // sum(SHARES)
        full, mine = polish(
            pair, core, start, size, ln_gain, ln_shift, gate_weight, gate_bias, out_gain, out_shift,
            out_weight, out_bias, triangle, full, step,
        )
        moving.append((start, swap(mine, "depth", 1)))
        start += size
    for start, arrived in moving:
        full = place(full, arrived, core, start, part, step)
    return full


def per_device(
    pair,
    ln_gain,
    ln_shift,
    proj_weight,
    proj_bias,
    gate_weight,
    gate_bias,
    out_gain,
    out_shift,
    out_weight,
    out_bias,
):
    rows_n, cols_n, depth_n = (lax.axis_size(a) for a in ("row", "col", "depth"))
    row, col, depth = (lax.axis_index(a) for a in ("row", "col", "depth"))
    rows, cols, channels = pair.shape
    hidden = proj_weight.shape[1] // 4
    low, high = col % 2, col // 2
    core = depth % 2
    per_depth = hidden // depth_n
    per_col = per_depth // 2
    step = per_col // CHUNKS
    half_j = 2 * cols
    part = cols // 2

    weight = proj_weight.T.reshape(4, hidden, channels)
    bias = proj_bias.reshape(4, hidden)
    first = depth * per_depth
    mine = lax.dynamic_slice_in_dim(weight, first, per_depth, 1)
    mine_bias = lax.dynamic_slice_in_dim(bias, first, per_depth, 1)
    mine = jnp.where(low == 0, mine, jnp.roll(mine, per_col, 1))
    mine_bias = jnp.where(low == 0, mine_bias, jnp.roll(mine_bias, per_col, 1))
    step_k = 16
    made = project_all(
        pair, ln_gain, ln_shift, mine.reshape(-1, channels), mine_bias.reshape(-1), 2 * CHUNKS, step_k
    )
    lefts, rights = made[: 2 * CHUNKS], made[2 * CHUNKS :]

    def gather_rows(right):
        if rows_n == 2:
            return pick(row == high, right, swap(right, "row", 1))
        whole = lax.all_gather(right, "row", axis=2, tiled=True)
        return (
            lax.dynamic_slice_in_dim(whole, high * half_j, half_j, 2),
            lax.dynamic_slice_in_dim(whole, (1 - high) * half_j, half_j, 2),
        )

    def contract(right, left):
        return jnp.einsum("hkj,hki->hji", right, left, preferred_element_type=jnp.float32)

    gathered = []
    far, crossed = [], []
    for chunk in range(CHUNKS):
        ahead = (lefts[CHUNKS + chunk], rights[CHUNKS + chunk])
        if chunk >= 2:
            *ahead, crossed[chunk - 2] = lax.optimization_barrier((*ahead, crossed[chunk - 2]))
        left_far, right_far = (swap(value, "col", 1) for value in ahead)
        far.append((left_far, gather_rows(rights[chunk]), gather_rows(right_far)))
        if chunk >= 1:
            crossed.append(cross_term(lefts, far, chunk - 1, contract))
    crossed.append(cross_term(lefts, far, CHUNKS - 1, contract))
    for chunk in range(CHUNKS):
        left_near = lefts[chunk]
        left_far, (near_own, _), (far_own, _) = far[chunk]
        arrived = swap(crossed[chunk], "col", 2)
        own = contract(near_own, left_near) + contract(far_own, left_far)
        triangle = (own + arrived.astype(jnp.float32)).astype(jnp.bfloat16)
        keep = lax.dynamic_slice_in_dim(triangle, low * cols, cols, 1)
        give = lax.dynamic_slice_in_dim(triangle, (1 - low) * cols, cols, 1)
        block = jnp.concatenate([keep, swap(give, "col", 1)], axis=0)
        same = lax.dynamic_slice_in_dim(block, core * part, part, 1)
        across = lax.dynamic_slice_in_dim(block, (1 - core) * part, part, 1)
        gathered += [
            same,
            swap(across, "depth", 1),
            swap(same, "depth", 2),
            swap(across, "depth", 3),
        ]

    order = jnp.concatenate(
        [
            (depth ^ m) * per_depth + (low ^ n) * per_col + chunk * step + jnp.arange(step)
            for chunk in range(CHUNKS)
            for m in range(4)
            for n in range(2)
        ]
    )
    finished = finish_all(
        pair,
        core,
        part,
        ln_gain,
        ln_shift,
        gate_weight,
        gate_bias,
        out_gain[order],
        out_shift[order],
        out_weight[order],
        out_bias,
        gathered,
        step_k,
    )
    first, second = pick(core == 0, finished, swap(finished, "depth", 1))
    return jnp.concatenate([first, second], axis=1)


def solution(mesh):
    placed = (P("row", "col", None), P(), P(), P(), P(), P(), P(), P(), P(), P(), P())
    small = tuple(mesh.shape[a] for a in ("row", "col", "depth")) == (2, 4, 4)
    return jax.shard_map(
        per_device_kernel if small else per_device, mesh=mesh, in_specs=placed, out_specs=P("row", "col", None), check_vma=False
    )
```

```python
import functools

import jax
import jax.numpy as jnp
from jax import lax
from jax.experimental import pallas as pl
from jax.experimental.pallas import tpu as pltpu
from jax.sharding import PartitionSpec as P

CHUNKS = 4
PIECES = 32
BUNCHES = 1
STATS_UNROLL = 8
NORM_UNROLL = 8
PROJECT_UNROLL = 16


def layer_norm(values, gain, shift):
    centre = jnp.mean(values, axis=-1, keepdims=True)
    centred = values - centre
    spread = jnp.mean(centred * centred, axis=-1, keepdims=True)
    return centred * lax.rsqrt(spread + 1e-05) * gain + shift


def wide_norm(values, gain, shift):
    channels = values.shape[-1]
    flat = values.reshape(-1, channels)
    level = jnp.full((channels, channels), 1.0 / channels, values.dtype)
    centre = jnp.dot(flat, level, preferred_element_type=jnp.float32)
    centred = flat.astype(jnp.float32) - centre
    spread = jnp.mean(centred * centred, axis=-1, keepdims=True)
    return (centred * lax.rsqrt(spread + 1e-05) * gain + shift).reshape(values.shape)


def flipped_dot(a, b):
    return lax.dot_general(a, b, (((1,), (1,)), ((), ())), preferred_element_type=jnp.float32)


def project_kernel(x_ref, gain_ref, shift_ref, w_ref, b_ref, *refs):
    outs, (flat, made) = refs[:-2], refs[-2:]
    rows, step_k, channels = x_ref.shape
    count = w_ref.shape[0] // 4
    each = outs[0].shape[0]
    normed = layer_norm(x_ref[...].astype(jnp.float32), gain_ref[...], shift_ref[...])
    flat[...] = normed.reshape(rows * step_k, channels)
    lanes = made.shape[2]
    for k in range(step_k):
        line = flat[pl.ds(k, rows, stride=step_k), :].astype(jnp.bfloat16)
        mixed = flipped_dot(w_ref[...], line) + b_ref[...]
        left = jax.nn.sigmoid(mixed[:count]) * mixed[count : 2 * count]
        right = jax.nn.sigmoid(mixed[2 * count : 3 * count]) * mixed[3 * count :]
        for side, value in enumerate((left, right)):
            for tile in range(rows // lanes):
                made[tile, pl.ds(side * count * step_k + k, count, stride=step_k), :] = value[
                    :, tile * lanes : (tile + 1) * lanes
                ]
    for n, out in enumerate(outs):
        for tile in range(rows // lanes):
            size = each * step_k
            out[:, :, tile * lanes : (tile + 1) * lanes] = (
                made[tile, n * size : (n + 1) * size, :]
                .reshape(each, step_k, lanes)
                .astype(jnp.bfloat16)
            )


def project_all(pair, gain, shift, weight, bias, pieces, step_k):
    rows, cols, channels = pair.shape
    count = weight.shape[0] // 4
    each = count // pieces
    lanes = 128 if rows % 128 == 0 else rows
    whole = lambda *shape: pl.BlockSpec(shape, lambda k: (0,) * len(shape))
    return pl.pallas_call(
        project_kernel,
        grid=(cols // step_k,),
        in_specs=[
            pl.BlockSpec((rows, step_k, channels), lambda k: (0, k, 0)),
            whole(1, channels),
            whole(1, channels),
            whole(4 * count, channels),
            whole(4 * count, 1),
        ],
        out_specs=[pl.BlockSpec((each, step_k, rows), lambda k: (0, k, 0))] * (2 * pieces),
        out_shape=[jax.ShapeDtypeStruct((each, cols, rows), jnp.bfloat16)] * (2 * pieces),
        scratch_shapes=[
            pltpu.VMEM((rows * step_k, channels), jnp.float32),
            pltpu.VMEM((rows // lanes, 2 * count * step_k, lanes), jnp.float32),
        ],
        compiler_params=pltpu.CompilerParams(vmem_limit_bytes=60 * 1024 * 1024),
        cost_estimate=pl.CostEstimate(
            flops=2 * rows * cols * channels * 4 * count,
            bytes_accessed=4 * rows * cols * channels,
            transcendentals=rows * cols * 2 * count,
        ),
    )(pair, gain[None], shift[None], weight, bias[:, None])


def finish_kernel(x_ref, gain_ref, shift_ref, gw_ref, gb_ref, og_ref, os_ref, ow_ref, ob_ref, *refs):
    tris, (out, held, done) = refs[:-3], refs[-3:]
    rows, step_j, channels = x_ref.shape
    hidden = ow_ref.shape[0]
    tiles, lanes = held.shape[0], held.shape[2]
    each = tris[0].shape[0]
    for tile in range(tiles):
        cut = slice(tile * lanes, (tile + 1) * lanes)
        total = 0.0
        for tri in tris:
            total = total + jnp.sum(tri[:, :, cut].astype(jnp.float32), axis=0)
        centre = total / hidden
        spread = 0.0
        for tri in tris:
            centred = tri[:, :, cut].astype(jnp.float32) - centre[None]
            spread = spread + jnp.sum(centred * centred, axis=0)
        scale = lax.rsqrt(spread / hidden + 1e-05)
        for n, tri in enumerate(tris):
            centred = tri[:, :, cut].astype(jnp.float32) - centre[None]
            held[tile, n * each * step_j : (n + 1) * each * step_j, :] = (
                centred * scale[None]
            ).reshape(each * step_j, lanes)
    for j in range(step_j):
        for tile in range(tiles):
            value = held[tile, pl.ds(j, hidden, stride=step_j), :]
            value = (value * og_ref[...] + os_ref[...]).astype(jnp.bfloat16)
            projected = lax.dot_general(
                value, ow_ref[...], (((0,), (0,)), ((), ())), preferred_element_type=jnp.float32
            )
            done[pl.ds(tile * lanes * step_j + j, lanes, stride=step_j), :] = projected
    normed = layer_norm(x_ref[...].astype(jnp.float32), gain_ref[...], shift_ref[...])
    flat = normed.reshape(rows * step_j, channels).astype(jnp.bfloat16)
    gate = jax.nn.sigmoid(
        jnp.dot(flat, gw_ref[...], preferred_element_type=jnp.float32) + gb_ref[...]
    )
    update = gate * (done[...] + ob_ref[...])
    out[...] = update.reshape(rows, step_j, channels).astype(jnp.bfloat16)


def finish_all(pair, core, part, gain, shift, gw, gb, og, os, ow, ob, tris, step_j):
    rows, _, channels = pair.shape
    hidden = ow.shape[0]
    lanes = 128 if rows % 128 == 0 else rows
    each = tris[0].shape[0]
    here = lax.dynamic_slice_in_dim(pair, core * part, part, 1)
    whole = lambda *shape: pl.BlockSpec(shape, lambda j: (0,) * len(shape))
    return pl.pallas_call(
        finish_kernel,
        grid=(part // step_j,),
        in_specs=[
            pl.BlockSpec((rows, step_j, channels), lambda j: (0, j, 0)),
            whole(1, channels),
            whole(1, channels),
            whole(channels, channels),
            whole(1, channels),
            whole(hidden, 1),
            whole(hidden, 1),
            whole(hidden, channels),
            whole(1, channels),
        ]
        + [pl.BlockSpec((each, step_j, rows), lambda j: (0, j, 0))] * len(tris),
        out_specs=pl.BlockSpec((rows, step_j, channels), lambda j: (0, j, 0)),
        out_shape=jax.ShapeDtypeStruct((rows, part, channels), jnp.bfloat16),
        scratch_shapes=[
            pltpu.VMEM((rows // lanes, hidden * step_j, lanes), jnp.float32),
            pltpu.VMEM((rows * step_j, channels), jnp.float32),
        ],
        compiler_params=pltpu.CompilerParams(vmem_limit_bytes=60 * 1024 * 1024),
        cost_estimate=pl.CostEstimate(
            flops=4 * rows * part * channels * channels,
            bytes_accessed=6 * rows * part * channels,
            transcendentals=rows * part * channels,
        ),
    )(here, gain[None], shift[None], gw, gb[None], og[:, None], os[:, None], ow, ob[None], *tris)


def exchange_kernel(
    pieces, pair, gain_ref, shift_ref, gw_ref, gb_ref, left, right, out, gates,
    lefts, rights, sent, arrived, blocks, seen, opened,
    local, edge_l, edge_r, near_sem, far_sem, cross_sem, give_sem, pass_sem, spread_sem, gone, seen_sem, opened_sem,
):
    row, col, depth = (lax.axis_index(a) for a in ("row", "col", "depth"))
    count, cols, rows = left.shape
    size = count // pieces
    inner = (col == 1) | (col == 2)
    low, high = col % 2, col // 2
    other = 1 - high
    mesh_id = pl.DeviceIdType.MESH
    over_row = (1 - row, col, depth)
    beside = (row, 2 * high + 1 - low, depth)
    opposite = (row, 3 - col, depth)
    peers = [(row, col, depth ^ m) for m in (1, 2)]

    def cut(t):
        return pl.ds(t * size, size)

    def remote(src, dst, kind, recv, device):
        return pltpu.make_async_remote_copy(
            src_ref=src, dst_ref=dst, send_sem=gone.at[kind], recv_sem=recv,
            device_id=device, device_id_type=mesh_id,
        )

    own_k, far_k = pl.ds(0, cols), pl.ds(cols, cols)

    def edge_left(t):
        return remote(left.at[cut(t)], lefts.at[cut(t), far_k], 0, edge_l.at[t], beside)

    def edge_right(t):
        return remote(right.at[cut(t)], rights.at[row, cut(t), far_k], 1, edge_r.at[t], beside)

    def near(t):
        return remote(right.at[cut(t)], rights.at[row, cut(t), own_k], 2, near_sem.at[t], over_row)

    def far(t):
        return remote(
            rights.at[row, cut(t), far_k], rights.at[row, cut(t), far_k], 3, far_sem.at[t], over_row
        )

    def cross(t):
        return remote(sent.at[cut(t)], arrived.at[cut(t)], 4, cross_sem.at[t], opposite)

    def give(t):
        return remote(
            blocks.at[1 - low, cut(t)], blocks.at[1 - low, cut(t)], 5, give_sem.at[t], beside
        )

    def spread(t):
        return remote(
            blocks.at[low, cut(t)], out.at[depth, cut(t)], 6, spread_sem.at[0], (row, col, depth ^ 1)
        )

    def hand(t):
        return remote(
            blocks.at[low, cut(t)], out.at[depth, cut(t)], 7, pass_sem.at[t], (row, col, depth ^ 2)
        )

    def onward(t):
        return remote(
            out.at[depth ^ 2, cut(t)], out.at[depth ^ 2, cut(t)], 8, spread_sem.at[1],
            (row, col, depth ^ 1),
        )

    def keep(t):
        return pltpu.make_async_copy(blocks.at[low, cut(t)], out.at[depth, cut(t)], local.at[2])

    def spread_all(t):
        hand(t).start()
        spread(t).start()
        keep(t).start()

        @pl.when(t >= 1)
        def _():
            relay(t - 1)

    def relay(t):
        hand(t).wait_recv()
        onward(t).start()

    def term(half, h):
        return lax.dot_general(
            rights[half, h], lefts[h], (((0,), (0,)), ((), ())), preferred_element_type=jnp.float32
        )

    bunch, step_j, channels = seen.shape[1:]
    across = rows // bunch
    units = across * (cols // step_j)
    speed = -(-units // pieces)

    def look(u):
        place = pl.multiple_of((u // across) * step_j, step_j)
        return pltpu.make_async_copy(
            pair.at[pl.ds((u % across) * bunch, bunch), pl.ds(place, step_j)],
            seen.at[u % 2],
            seen_sem.at[u % 2],
        )

    def show(u):
        place = pl.multiple_of((u // across) * step_j, step_j)
        return pltpu.make_async_copy(
            opened.at[u % 2],
            gates.at[pl.ds((u % across) * bunch, bunch), pl.ds(place, step_j)],
            opened_sem.at[u % 2],
        )

    def open_gate(u):
        @pl.when(u < units)
        def _():
            look(u).wait()

            @pl.when(u + 1 < units)
            def _():
                look(u + 1).start()

            @pl.when(u >= 2)
            def _():
                show(u - 2).wait()

            normed = layer_norm(seen[u % 2].astype(jnp.float32), gain_ref[...], shift_ref[...])
            flat = normed.reshape(bunch * step_j, channels).astype(jnp.bfloat16)
            gate = jax.nn.sigmoid(
                jnp.dot(flat, gw_ref[...], preferred_element_type=jnp.float32) + gb_ref[...]
            )
            opened[u % 2] = gate.reshape(bunch, step_j, channels)
            show(u).start()

    def open_gates(t):
        for n in range(speed):
            open_gate(t * speed + n)

    look(0).start()
    barrier = pltpu.get_barrier_semaphore()
    for device in (over_row, beside, opposite, *peers):
        pl.semaphore_signal(barrier, inc=1, device_id=device, device_id_type=mesh_id)
    pl.semaphore_wait(barrier, 5)

    @pl.when(inner)
    def _():
        load_l = pltpu.make_async_copy(left, lefts.at[:, own_k], local.at[0])
        load_r = pltpu.make_async_copy(right, rights.at[row, :, own_k], local.at[1])
        near(0).start()
        load_l.start()
        load_r.start()
        near(1).start()
        load_l.wait()
        load_r.wait()

        def meet(t):
            near(t).wait_recv()
            far(t).wait_recv()

        def step(t, _):
            @pl.when(t < pieces)
            def _():
                edge_left(t).wait_recv()
                edge_right(t).wait_recv()
                far(t).start()

                @pl.when(t + 2 < pieces)
                def _():
                    near(t + 2).start()

                @pl.when(row != other)
                def _():
                    meet(t)

                def one(h, _):
                    sent[t * size + h] = term(other, t * size + h).astype(jnp.bfloat16)
                    return 0

                lax.fori_loop(0, size, one, 0)
                cross(t).start()

            open_gates(t)

            @pl.when(t >= 1)
            def _():
                u = t - 1

                @pl.when(row == other)
                def _():
                    meet(u)

                cross(u).wait_recv()

                def one(h, _):
                    h = u * size + h
                    total = (term(high, h) + arrived[h].astype(jnp.float32)).astype(jnp.bfloat16)
                    blocks[0, h] = total[:cols]
                    blocks[1, h] = total[cols:]
                    return 0

                lax.fori_loop(0, size, one, 0)
                give(u).start()
                spread_all(u)

            return 0

        lax.fori_loop(0, pieces + 1, step, 0)
        whole = blocks.at[0]
        for kind in (2, 3, 5):
            pltpu.make_async_copy(whole, whole, gone.at[kind]).wait()
        pltpu.make_async_copy(sent, sent, gone.at[4]).wait()

    @pl.when(jnp.logical_not(inner))
    def _():
        def push(t, _):
            edge_left(t).start()
            edge_right(t).start()
            return 0

        lax.fori_loop(0, pieces, push, 0)

        def step(t, _):
            open_gates(t)
            give(t).wait_recv()
            spread_all(t)
            return 0

        lax.fori_loop(0, pieces, step, 0)
        pltpu.make_async_copy(left, left, gone.at[0]).wait()
        pltpu.make_async_copy(right, right, gone.at[1]).wait()

    relay(pieces - 1)
    for u in range(max(units - 2, 0), units):
        show(u).wait()
    mine = out.at[depth]
    pltpu.make_async_copy(mine, mine, local.at[2]).wait()
    for kind in (6, 7, 8):
        pltpu.make_async_copy(mine, mine, gone.at[kind]).wait()
    for n in range(2):
        pltpu.make_async_copy(mine, mine, spread_sem.at[n]).wait()


def exchange(pair, gain, shift, gw, gb, left, right, pieces, step_j):
    count, cols, rows = left.shape
    channels = pair.shape[2]
    bunch = rows // 4
    dma = pltpu.SemaphoreType.DMA
    anywhere = pl.BlockSpec(memory_space=pl.ANY)
    return pl.pallas_call(
        functools.partial(exchange_kernel, pieces),
        in_specs=[anywhere] + [pl.BlockSpec(memory_space=pltpu.VMEM)] * 4 + [anywhere] * 2,
        out_specs=[anywhere, anywhere],
        out_shape=[
            jax.ShapeDtypeStruct((4, count, cols, rows), jnp.bfloat16),
            jax.ShapeDtypeStruct((rows, cols, channels), jnp.float32),
        ],
        scratch_shapes=[
            pltpu.VMEM((count, 2 * cols, rows), jnp.bfloat16),
            pltpu.VMEM((2, count, 2 * cols, rows), jnp.bfloat16),
            pltpu.VMEM((count, rows, rows), jnp.bfloat16),
            pltpu.VMEM((count, rows, rows), jnp.bfloat16),
            pltpu.VMEM((2, count, cols, rows), jnp.bfloat16),
            pltpu.VMEM((2, bunch, step_j, channels), jnp.bfloat16),
            pltpu.VMEM((2, bunch, step_j, channels), jnp.float32),
            dma((3,)),
        ]
        + [dma((pieces,))] * 7
        + [dma((2,)), dma((9,)), dma((2,)), dma((2,))],
        compiler_params=pltpu.CompilerParams(
            collective_id=0, has_side_effects=True, vmem_limit_bytes=63 * 1024 * 1024
        ),
        name="exchange",
    )(pair, gain[None], shift[None], gw, gb[None], left, right)


PITCH = 17


def polish_kernel(gate_ref, og_ref, os_ref, ow_ref, ob_ref, tri_ref, out, held, done):
    rows, step_j, channels = gate_ref.shape
    hidden = tri_ref.shape[0]
    tiles, lanes = held.shape[0], held.shape[2]
    group = 16
    for tile in range(tiles):
        cut = slice(tile * lanes, (tile + 1) * lanes)

        def block(g):
            return tri_ref[pl.ds(g * group, group), :, cut].astype(jnp.float32)

        zero = jnp.zeros((step_j, lanes), jnp.float32)
        first = tri_ref[0, :, cut].astype(jnp.float32)

        def gauge(g, sums):
            moved = block(g) - first[None]
            return sums[0] + jnp.sum(moved, axis=0), sums[1] + jnp.sum(moved * moved, axis=0)

        total, power = lax.fori_loop(0, hidden // group, gauge, (zero, zero), unroll=STATS_UNROLL)
        shift = total / hidden
        centre = first + shift
        spread = jnp.maximum(power - total * shift, 0.0)
        scale = lax.rsqrt(spread / hidden + 1e-05)

        def normalise(g, _):
            for n in range(group):
                h = g * group + n
                value = (tri_ref[h, :, cut].astype(jnp.float32) - centre) * scale
                held[tile, pl.ds(h * PITCH, step_j), :] = value * og_ref[h] + os_ref[h]
            return 0

        lax.fori_loop(0, hidden // group, normalise, 0, unroll=NORM_UNROLL)

    def project(j, _):
        for tile in range(tiles):
            value = held[tile, pl.ds(j, hidden, stride=PITCH), :].astype(jnp.bfloat16)
            done[pl.ds(tile * lanes * PITCH + j, lanes, stride=PITCH), :] = lax.dot_general(
                value, ow_ref[...], (((0,), (0,)), ((), ())), preferred_element_type=jnp.float32
            )
        return 0

    lax.fori_loop(0, step_j, project, 0, unroll=PROJECT_UNROLL)
    bunch = 32

    def close(g, _):
        for n in range(bunch):
            at = g * bunch + n
            update = gate_ref[at] * (done[pl.ds(at * PITCH, step_j), :] + ob_ref[...])
            out[at] = update.astype(jnp.bfloat16)
        return 0

    lax.fori_loop(0, rows // bunch, close, 0)


def polish(gates, og, os, ow, ob, tri, step_j):
    rows, cols, channels = gates.shape
    hidden = tri.shape[0]
    lanes = 128 if rows % 128 == 0 else rows
    whole = lambda *shape: pl.BlockSpec(shape, lambda j: (0,) * len(shape))
    scalars = pl.BlockSpec(memory_space=pltpu.SMEM)
    moved = pl.BlockSpec((rows, step_j, channels), lambda j: (0, j, 0))
    return pl.pallas_call(
        polish_kernel,
        grid=(cols // step_j,),
        in_specs=[
            moved,
            scalars,
            scalars,
            whole(hidden, channels),
            whole(1, channels),
            pl.BlockSpec((hidden, step_j, rows), lambda j: (0, j, 0)),
        ],
        out_specs=moved,
        out_shape=jax.ShapeDtypeStruct((rows, cols, channels), jnp.bfloat16),
        scratch_shapes=[
            pltpu.VMEM((rows // lanes, hidden * PITCH, lanes), jnp.float32),
            pltpu.VMEM((rows * PITCH, channels), jnp.float32),
        ],
        compiler_params=pltpu.CompilerParams(vmem_limit_bytes=60 * 1024 * 1024),
        name="polish",
    )(gates, og, os, ow, ob[None], tri)


def spread_kernel(x_ref, gain_ref, shift_ref, w_ref, b_ref, left_ref, right_ref, flat, made):
    rows, step_k, channels = x_ref.shape
    count = left_ref.shape[0]
    tiles, _, lanes = made.shape
    tall = rows + 1
    bunch = rows // BUNCHES

    def normalise(g, _):
        normed = wide_norm(x_ref[pl.ds(g * bunch, bunch)], gain_ref[...], shift_ref[...])
        for n in range(bunch):
            for k in range(0, step_k, 8):
                flat[pl.ds(k * tall + g * bunch + n, 8, stride=tall), :] = normed[n, k : k + 8]
        return 0

    lax.fori_loop(0, BUNCHES, normalise, 0)

    def mix(k, _):
        line = flat[pl.ds(k * tall, rows), :].astype(jnp.bfloat16)
        mixed = flipped_dot(w_ref[...], line) + b_ref[...]
        for side in range(2):
            base = 2 * side * count
            value = jax.nn.sigmoid(mixed[base : base + count]) * mixed[base + count : base + 2 * count]
            for tile in range(tiles):
                made[tile, pl.ds(side * count * PITCH + k, count, stride=PITCH), :] = value[
                    :, tile * lanes : (tile + 1) * lanes
                ]
        return 0

    lax.fori_loop(0, step_k, mix, 0, unroll=16)

    def put(h, _):
        for tile in range(tiles):
            cut = slice(tile * lanes, (tile + 1) * lanes)
            for side, out in enumerate((left_ref, right_ref)):
                out[h, :, cut] = made[
                    tile, pl.ds((side * count + h) * PITCH, step_k), :
                ].astype(jnp.bfloat16)
        return 0

    lax.fori_loop(0, count, put, 0, unroll=4)


def project_pair(pair, gain, shift, weight, bias, step_k):
    rows, cols, channels = pair.shape
    count = weight.shape[0] // 4
    lanes = 128 if rows % 128 == 0 else rows
    whole = lambda *shape: pl.BlockSpec(shape, lambda k: (0,) * len(shape))
    return pl.pallas_call(
        spread_kernel,
        grid=(cols // step_k,),
        in_specs=[
            pl.BlockSpec((rows, step_k, channels), lambda k: (0, k, 0)),
            whole(1, channels),
            whole(1, channels),
            whole(4 * count, channels),
            whole(4 * count, 1),
        ],
        out_specs=[pl.BlockSpec((count, step_k, rows), lambda k: (0, k, 0))] * 2,
        out_shape=[jax.ShapeDtypeStruct((count, cols, rows), jnp.bfloat16)] * 2,
        scratch_shapes=[
            pltpu.VMEM((step_k * (rows + 1), channels), jnp.float32),
            pltpu.VMEM((rows // lanes, 2 * count * PITCH, lanes), jnp.float32),
        ],
        compiler_params=pltpu.CompilerParams(vmem_limit_bytes=60 * 1024 * 1024),
        name="project",
    )(pair, gain[None], shift[None], weight, bias[:, None])


def swap(value, axis, bit):
    count = lax.axis_size(axis)
    return lax.ppermute(value, axis, [(n, n ^ bit) for n in range(count)])


def pick(first_mine, mine, other):
    return jnp.where(first_mine, mine, other), jnp.where(first_mine, other, mine)


def cross_term(lefts, far, chunk, contract):
    left_far, (_, near), (_, beyond) = far[chunk]
    return (contract(near, lefts[chunk]) + contract(beyond, left_far)).astype(jnp.bfloat16)


def per_device_kernel(
    pair,
    ln_gain,
    ln_shift,
    proj_weight,
    proj_bias,
    gate_weight,
    gate_bias,
    out_gain,
    out_shift,
    out_weight,
    out_bias,
):
    depth_n = lax.axis_size("depth")
    depth = lax.axis_index("depth")
    rows, cols, channels = pair.shape
    hidden = proj_weight.shape[1] // 4
    per_depth = hidden // depth_n
    step = 16
    weight = proj_weight.T.reshape(4, hidden, channels)
    bias = proj_bias.reshape(4, hidden)
    mine = lax.dynamic_slice_in_dim(weight, depth * per_depth, per_depth, 1)
    mine_bias = lax.dynamic_slice_in_dim(bias, depth * per_depth, per_depth, 1)
    left, right = project_pair(
        pair, ln_gain, ln_shift, mine.reshape(-1, channels), mine_bias.reshape(-1), step
    )
    triangle, gates = exchange(
        pair, ln_gain, ln_shift, gate_weight, gate_bias, left, right, PIECES, step
    )
    triangle = triangle.reshape(hidden, cols, rows)
    return polish(gates, out_gain, out_shift, out_weight, out_bias, triangle, step)


def per_device(
    pair,
    ln_gain,
    ln_shift,
    proj_weight,
    proj_bias,
    gate_weight,
    gate_bias,
    out_gain,
    out_shift,
    out_weight,
    out_bias,
):
    rows_n, cols_n, depth_n = (lax.axis_size(a) for a in ("row", "col", "depth"))
    row, col, depth = (lax.axis_index(a) for a in ("row", "col", "depth"))
    rows, cols, channels = pair.shape
    hidden = proj_weight.shape[1] // 4
    low, high = col % 2, col // 2
    core = depth % 2
    per_depth = hidden // depth_n
    per_col = per_depth // 2
    step = per_col // CHUNKS
    half_j = 2 * cols
    part = cols // 2

    weight = proj_weight.T.reshape(4, hidden, channels)
    bias = proj_bias.reshape(4, hidden)
    first = depth * per_depth
    mine = lax.dynamic_slice_in_dim(weight, first, per_depth, 1)
    mine_bias = lax.dynamic_slice_in_dim(bias, first, per_depth, 1)
    mine = jnp.where(low == 0, mine, jnp.roll(mine, per_col, 1))
    mine_bias = jnp.where(low == 0, mine_bias, jnp.roll(mine_bias, per_col, 1))
    step_k = 16
    made = project_all(
        pair, ln_gain, ln_shift, mine.reshape(-1, channels), mine_bias.reshape(-1), 2 * CHUNKS, step_k
    )
    lefts, rights = made[: 2 * CHUNKS], made[2 * CHUNKS :]

    def gather_rows(right):
        if rows_n == 2:
            return pick(row == high, right, swap(right, "row", 1))
        whole = lax.all_gather(right, "row", axis=2, tiled=True)
        return (
            lax.dynamic_slice_in_dim(whole, high * half_j, half_j, 2),
            lax.dynamic_slice_in_dim(whole, (1 - high) * half_j, half_j, 2),
        )

    def contract(right, left):
        return jnp.einsum("hkj,hki->hji", right, left, preferred_element_type=jnp.float32)

    gathered = []
    far, crossed = [], []
    for chunk in range(CHUNKS):
        ahead = (lefts[CHUNKS + chunk], rights[CHUNKS + chunk])
        if chunk >= 2:
            *ahead, crossed[chunk - 2] = lax.optimization_barrier((*ahead, crossed[chunk - 2]))
        left_far, right_far = (swap(value, "col", 1) for value in ahead)
        far.append((left_far, gather_rows(rights[chunk]), gather_rows(right_far)))
        if chunk >= 1:
            crossed.append(cross_term(lefts, far, chunk - 1, contract))
    crossed.append(cross_term(lefts, far, CHUNKS - 1, contract))
    for chunk in range(CHUNKS):
        left_near = lefts[chunk]
        left_far, (near_own, _), (far_own, _) = far[chunk]
        arrived = swap(crossed[chunk], "col", 2)
        own = contract(near_own, left_near) + contract(far_own, left_far)
        triangle = (own + arrived.astype(jnp.float32)).astype(jnp.bfloat16)
        keep = lax.dynamic_slice_in_dim(triangle, low * cols, cols, 1)
        give = lax.dynamic_slice_in_dim(triangle, (1 - low) * cols, cols, 1)
        block = jnp.concatenate([keep, swap(give, "col", 1)], axis=0)
        same = lax.dynamic_slice_in_dim(block, core * part, part, 1)
        across = lax.dynamic_slice_in_dim(block, (1 - core) * part, part, 1)
        gathered += [
            same,
            swap(across, "depth", 1),
            swap(same, "depth", 2),
            swap(across, "depth", 3),
        ]

    order = jnp.concatenate(
        [
            (depth ^ m) * per_depth + (low ^ n) * per_col + chunk * step + jnp.arange(step)
            for chunk in range(CHUNKS)
            for m in range(4)
            for n in range(2)
        ]
    )
    finished = finish_all(
        pair,
        core,
        part,
        ln_gain,
        ln_shift,
        gate_weight,
        gate_bias,
        out_gain[order],
        out_shift[order],
        out_weight[order],
        out_bias,
        gathered,
        step_k,
    )
    first, second = pick(core == 0, finished, swap(finished, "depth", 1))
    return jnp.concatenate([first, second], axis=1)


def solution(mesh):
    placed = (P("row", "col", None), P(), P(), P(), P(), P(), P(), P(), P(), P(), P())
    small = tuple(mesh.shape[a] for a in ("row", "col", "depth")) == (2, 4, 4)
    return jax.shard_map(
        per_device_kernel if small else per_device, mesh=mesh, in_specs=placed, out_specs=P("row", "col", None), check_vma=False
    )
```

```python
import functools

import jax
import jax.numpy as jnp
from jax import lax
from jax.experimental import pallas as pl
from jax.experimental.pallas import tpu as pltpu
from jax.sharding import PartitionSpec as P

CHUNKS = 4
PIECES = 32
BUNCHES = 1
STATS_UNROLL = 8
NORM_UNROLL = 8
PROJECT_UNROLL = 16


def layer_norm(values, gain, shift):
    centre = jnp.mean(values, axis=-1, keepdims=True)
    centred = values - centre
    spread = jnp.mean(centred * centred, axis=-1, keepdims=True)
    return centred * lax.rsqrt(spread + 1e-05) * gain + shift


def wide_norm(values, gain, shift):
    channels = values.shape[-1]
    flat = values.reshape(-1, channels)
    level = jnp.full((channels, channels), 1.0 / channels, values.dtype)
    centre = jnp.dot(flat, level, preferred_element_type=jnp.float32)
    centred = flat.astype(jnp.float32) - centre
    spread = jnp.mean(centred * centred, axis=-1, keepdims=True)
    return (centred * lax.rsqrt(spread + 1e-05) * gain + shift).reshape(values.shape)


def flipped_dot(a, b):
    return lax.dot_general(a, b, (((1,), (1,)), ((), ())), preferred_element_type=jnp.float32)


def project_kernel(x_ref, gain_ref, shift_ref, w_ref, b_ref, *refs):
    outs, (flat, made) = refs[:-2], refs[-2:]
    rows, step_k, channels = x_ref.shape
    count = w_ref.shape[0] // 4
    each = outs[0].shape[0]
    normed = layer_norm(x_ref[...].astype(jnp.float32), gain_ref[...], shift_ref[...])
    flat[...] = normed.reshape(rows * step_k, channels)
    lanes = made.shape[2]
    for k in range(step_k):
        line = flat[pl.ds(k, rows, stride=step_k), :].astype(jnp.bfloat16)
        mixed = flipped_dot(w_ref[...], line) + b_ref[...]
        left = jax.nn.sigmoid(mixed[:count]) * mixed[count : 2 * count]
        right = jax.nn.sigmoid(mixed[2 * count : 3 * count]) * mixed[3 * count :]
        for side, value in enumerate((left, right)):
            for tile in range(rows // lanes):
                made[tile, pl.ds(side * count * step_k + k, count, stride=step_k), :] = value[
                    :, tile * lanes : (tile + 1) * lanes
                ]
    for n, out in enumerate(outs):
        for tile in range(rows // lanes):
            size = each * step_k
            out[:, :, tile * lanes : (tile + 1) * lanes] = (
                made[tile, n * size : (n + 1) * size, :]
                .reshape(each, step_k, lanes)
                .astype(jnp.bfloat16)
            )


def project_all(pair, gain, shift, weight, bias, pieces, step_k):
    rows, cols, channels = pair.shape
    count = weight.shape[0] // 4
    each = count // pieces
    lanes = 128 if rows % 128 == 0 else rows
    whole = lambda *shape: pl.BlockSpec(shape, lambda k: (0,) * len(shape))
    return pl.pallas_call(
        project_kernel,
        grid=(cols // step_k,),
        in_specs=[
            pl.BlockSpec((rows, step_k, channels), lambda k: (0, k, 0)),
            whole(1, channels),
            whole(1, channels),
            whole(4 * count, channels),
            whole(4 * count, 1),
        ],
        out_specs=[pl.BlockSpec((each, step_k, rows), lambda k: (0, k, 0))] * (2 * pieces),
        out_shape=[jax.ShapeDtypeStruct((each, cols, rows), jnp.bfloat16)] * (2 * pieces),
        scratch_shapes=[
            pltpu.VMEM((rows * step_k, channels), jnp.float32),
            pltpu.VMEM((rows // lanes, 2 * count * step_k, lanes), jnp.float32),
        ],
        compiler_params=pltpu.CompilerParams(vmem_limit_bytes=60 * 1024 * 1024),
        cost_estimate=pl.CostEstimate(
            flops=2 * rows * cols * channels * 4 * count,
            bytes_accessed=4 * rows * cols * channels,
            transcendentals=rows * cols * 2 * count,
        ),
    )(pair, gain[None], shift[None], weight, bias[:, None])


def finish_kernel(x_ref, gain_ref, shift_ref, gw_ref, gb_ref, og_ref, os_ref, ow_ref, ob_ref, *refs):
    tris, (out, held, done) = refs[:-3], refs[-3:]
    rows, step_j, channels = x_ref.shape
    hidden = ow_ref.shape[0]
    tiles, lanes = held.shape[0], held.shape[2]
    each = tris[0].shape[0]
    for tile in range(tiles):
        cut = slice(tile * lanes, (tile + 1) * lanes)
        total = 0.0
        for tri in tris:
            total = total + jnp.sum(tri[:, :, cut].astype(jnp.float32), axis=0)
        centre = total / hidden
        spread = 0.0
        for tri in tris:
            centred = tri[:, :, cut].astype(jnp.float32) - centre[None]
            spread = spread + jnp.sum(centred * centred, axis=0)
        scale = lax.rsqrt(spread / hidden + 1e-05)
        for n, tri in enumerate(tris):
            centred = tri[:, :, cut].astype(jnp.float32) - centre[None]
            held[tile, n * each * step_j : (n + 1) * each * step_j, :] = (
                centred * scale[None]
            ).reshape(each * step_j, lanes)
    for j in range(step_j):
        for tile in range(tiles):
            value = held[tile, pl.ds(j, hidden, stride=step_j), :]
            value = (value * og_ref[...] + os_ref[...]).astype(jnp.bfloat16)
            projected = lax.dot_general(
                value, ow_ref[...], (((0,), (0,)), ((), ())), preferred_element_type=jnp.float32
            )
            done[pl.ds(tile * lanes * step_j + j, lanes, stride=step_j), :] = projected
    normed = layer_norm(x_ref[...].astype(jnp.float32), gain_ref[...], shift_ref[...])
    flat = normed.reshape(rows * step_j, channels).astype(jnp.bfloat16)
    gate = jax.nn.sigmoid(
        jnp.dot(flat, gw_ref[...], preferred_element_type=jnp.float32) + gb_ref[...]
    )
    update = gate * (done[...] + ob_ref[...])
    out[...] = update.reshape(rows, step_j, channels).astype(jnp.bfloat16)


def finish_all(pair, core, part, gain, shift, gw, gb, og, os, ow, ob, tris, step_j):
    rows, _, channels = pair.shape
    hidden = ow.shape[0]
    lanes = 128 if rows % 128 == 0 else rows
    each = tris[0].shape[0]
    here = lax.dynamic_slice_in_dim(pair, core * part, part, 1)
    whole = lambda *shape: pl.BlockSpec(shape, lambda j: (0,) * len(shape))
    return pl.pallas_call(
        finish_kernel,
        grid=(part // step_j,),
        in_specs=[
            pl.BlockSpec((rows, step_j, channels), lambda j: (0, j, 0)),
            whole(1, channels),
            whole(1, channels),
            whole(channels, channels),
            whole(1, channels),
            whole(hidden, 1),
            whole(hidden, 1),
            whole(hidden, channels),
            whole(1, channels),
        ]
        + [pl.BlockSpec((each, step_j, rows), lambda j: (0, j, 0))] * len(tris),
        out_specs=pl.BlockSpec((rows, step_j, channels), lambda j: (0, j, 0)),
        out_shape=jax.ShapeDtypeStruct((rows, part, channels), jnp.bfloat16),
        scratch_shapes=[
            pltpu.VMEM((rows // lanes, hidden * step_j, lanes), jnp.float32),
            pltpu.VMEM((rows * step_j, channels), jnp.float32),
        ],
        compiler_params=pltpu.CompilerParams(vmem_limit_bytes=60 * 1024 * 1024),
        cost_estimate=pl.CostEstimate(
            flops=4 * rows * part * channels * channels,
            bytes_accessed=6 * rows * part * channels,
            transcendentals=rows * part * channels,
        ),
    )(here, gain[None], shift[None], gw, gb[None], og[:, None], os[:, None], ow, ob[None], *tris)


def exchange_kernel(
    pieces, pair, gain_ref, shift_ref, gw_ref, gb_ref, left, right, out, gates,
    lefts, rights, sent, arrived, blocks, seen, opened, base,
    local, edge_l, edge_r, near_sem, far_sem, cross_sem, late_sem, give_sem, pass_sem, spread_sem, gone, seen_sem, opened_sem,
):
    row, col, depth = (lax.axis_index(a) for a in ("row", "col", "depth"))
    count, cols, rows = left.shape
    size = count // pieces
    inner = (col == 1) | (col == 2)
    low, high = col % 2, col // 2
    other = 1 - high
    mesh_id = pl.DeviceIdType.MESH
    over_row = (1 - row, col, depth)
    beside = (row, 2 * high + 1 - low, depth)
    opposite = (row, 3 - col, depth)
    peers = [(row, col, depth ^ m) for m in (1, 2)]

    def cut(t):
        return pl.ds(t * size, size)

    def remote(src, dst, kind, recv, device):
        return pltpu.make_async_remote_copy(
            src_ref=src, dst_ref=dst, send_sem=gone.at[kind], recv_sem=recv,
            device_id=device, device_id_type=mesh_id,
        )

    own_k, far_k = pl.ds(0, cols), pl.ds(cols, cols)

    def edge_left(t):
        return remote(left.at[cut(t)], lefts.at[cut(t), far_k], 0, edge_l.at[t], beside)

    def edge_right(t):
        return remote(right.at[cut(t)], rights.at[row, cut(t), far_k], 1, edge_r.at[t], beside)

    def near(t):
        return remote(right.at[cut(t)], rights.at[row, cut(t), own_k], 2, near_sem.at[t], over_row)

    def far(t):
        return remote(
            rights.at[row, cut(t), far_k], rights.at[row, cut(t), far_k], 3, far_sem.at[t], over_row
        )

    def cross(t):
        return remote(sent.at[cut(t), low], arrived.at[cut(t), low], 4, cross_sem.at[t], opposite)

    def cross_late(t):
        return remote(
            sent.at[cut(t), 1 - low], arrived.at[cut(t), 1 - low], 4, late_sem.at[t], opposite
        )

    def give(t):
        return remote(
            blocks.at[1 - low, cut(t)], blocks.at[1 - low, cut(t)], 5, give_sem.at[t], beside
        )

    def spread(t):
        return remote(
            blocks.at[low, cut(t)], out.at[depth, cut(t)], 6, spread_sem.at[0], (row, col, depth ^ 1)
        )

    def hand(t):
        return remote(
            blocks.at[low, cut(t)], out.at[depth, cut(t)], 7, pass_sem.at[t], (row, col, depth ^ 2)
        )

    def onward(t):
        return remote(
            out.at[depth ^ 2, cut(t)], out.at[depth ^ 2, cut(t)], 8, spread_sem.at[1],
            (row, col, depth ^ 1),
        )

    def keep(t):
        return pltpu.make_async_copy(blocks.at[low, cut(t)], out.at[depth, cut(t)], local.at[2])

    def spread_all(t):
        hand(t).start()
        spread(t).start()
        keep(t).start()

        @pl.when(t >= 1)
        def _():
            relay(t - 1)

    def relay(t):
        hand(t).wait_recv()
        onward(t).start()

    def term(half, h):
        return lax.dot_general(
            rights[half, h], lefts[h], (((0,), (0,)), ((), ())), preferred_element_type=jnp.float32
        )

    bunch, step_j, channels = seen.shape[1:]
    across = rows // bunch
    units = across * (cols // step_j)
    speed = -(-units // pieces)

    def look(u):
        place = pl.multiple_of((u // across) * step_j, step_j)
        return pltpu.make_async_copy(
            pair.at[pl.ds((u % across) * bunch, bunch), pl.ds(place, step_j)],
            seen.at[u % 2],
            seen_sem.at[u % 2],
        )

    def show(u):
        place = pl.multiple_of((u // across) * step_j, step_j)
        return pltpu.make_async_copy(
            opened.at[u % 2],
            gates.at[pl.ds((u % across) * bunch, bunch), pl.ds(place, step_j)],
            opened_sem.at[u % 2],
        )

    def open_gate(u):
        @pl.when(u < units)
        def _():
            look(u).wait()

            @pl.when(u + 1 < units)
            def _():
                look(u + 1).start()

            @pl.when(u >= 2)
            def _():
                show(u - 2).wait()

            normed = layer_norm(seen[u % 2].astype(jnp.float32), gain_ref[...], shift_ref[...])
            flat = normed.reshape(bunch * step_j, channels).astype(jnp.bfloat16)
            gate = jax.nn.sigmoid(
                jnp.dot(flat, gw_ref[...], preferred_element_type=jnp.float32) + gb_ref[...]
            )
            opened[u % 2] = gate.reshape(bunch, step_j, channels)
            show(u).start()

    def open_gates(t):
        for n in range(speed):
            open_gate(t * speed + n)

    look(0).start()
    barrier = pltpu.get_barrier_semaphore()
    for device in (over_row, beside, opposite, *peers):
        pl.semaphore_signal(barrier, inc=1, device_id=device, device_id_type=mesh_id)
    pl.semaphore_wait(barrier, 5)

    @pl.when(inner)
    def _():
        load_l = pltpu.make_async_copy(left, lefts.at[:, own_k], local.at[0])
        load_r = pltpu.make_async_copy(right, rights.at[row, :, own_k], local.at[1])
        near(0).start()
        load_l.start()
        load_r.start()
        near(1).start()
        load_l.wait()
        load_r.wait()

        def meet(t):
            near(t).wait_recv()
            far(t).wait_recv()

        def step(t, _):
            @pl.when(t < pieces)
            def _():
                edge_left(t).wait_recv()
                edge_right(t).wait_recv()
                far(t).start()

                @pl.when(t + 2 < pieces)
                def _():
                    near(t + 2).start()

                @pl.when(row != other)
                def _():
                    meet(t)

                def one(h, _):
                    total = term(other, t * size + h).astype(jnp.bfloat16)
                    sent[t * size + h, 0] = total[:cols]
                    sent[t * size + h, 1] = total[cols:]
                    return 0

                lax.fori_loop(0, size, one, 0)
                cross(t).start()
                cross_late(t).start()

            open_gates(t)

            @pl.when(t >= 1)
            def _():
                u = t - 1

                @pl.when(row == other)
                def _():
                    meet(u)

                def one(h, _):
                    total = term(high, u * size + h)
                    base[h, 0] = total[:cols]
                    base[h, 1] = total[cols:]
                    return 0

                lax.fori_loop(0, size, one, 0)

                def add(place):
                    def each(h, _):
                        more = arrived[u * size + h, place].astype(jnp.float32)
                        blocks[place, u * size + h] = (base[h, place] + more).astype(jnp.bfloat16)
                        return 0

                    lax.fori_loop(0, size, each, 0)

                cross(u).wait_recv()
                add(1 - low)
                give(u).start()
                cross_late(u).wait_recv()
                add(low)
                spread_all(u)

            return 0

        lax.fori_loop(0, pieces + 1, step, 0)
        whole = blocks.at[0]
        for kind in (2, 3, 5):
            pltpu.make_async_copy(whole, whole, gone.at[kind]).wait()
        pltpu.make_async_copy(sent, sent, gone.at[4]).wait()

    @pl.when(jnp.logical_not(inner))
    def _():
        def push(t, _):
            edge_left(t).start()
            edge_right(t).start()
            return 0

        lax.fori_loop(0, pieces, push, 0)

        def step(t, _):
            open_gates(t)
            give(t).wait_recv()
            spread_all(t)
            return 0

        lax.fori_loop(0, pieces, step, 0)
        pltpu.make_async_copy(left, left, gone.at[0]).wait()
        pltpu.make_async_copy(right, right, gone.at[1]).wait()

    relay(pieces - 1)
    for u in range(max(units - 2, 0), units):
        show(u).wait()
    mine = out.at[depth]
    pltpu.make_async_copy(mine, mine, local.at[2]).wait()
    for kind in (6, 7, 8):
        pltpu.make_async_copy(mine, mine, gone.at[kind]).wait()
    for n in range(2):
        pltpu.make_async_copy(mine, mine, spread_sem.at[n]).wait()


def exchange(pair, gain, shift, gw, gb, left, right, pieces, step_j):
    count, cols, rows = left.shape
    channels = pair.shape[2]
    bunch = rows // 4
    dma = pltpu.SemaphoreType.DMA
    anywhere = pl.BlockSpec(memory_space=pl.ANY)
    return pl.pallas_call(
        functools.partial(exchange_kernel, pieces),
        in_specs=[anywhere] + [pl.BlockSpec(memory_space=pltpu.VMEM)] * 4 + [anywhere] * 2,
        out_specs=[anywhere, anywhere],
        out_shape=[
            jax.ShapeDtypeStruct((4, count, cols, rows), jnp.bfloat16),
            jax.ShapeDtypeStruct((rows, cols, channels), jnp.float32),
        ],
        scratch_shapes=[
            pltpu.VMEM((count, 2 * cols, rows), jnp.bfloat16),
            pltpu.VMEM((2, count, 2 * cols, rows), jnp.bfloat16),
            pltpu.VMEM((count, 2, cols, rows), jnp.bfloat16),
            pltpu.VMEM((count, 2, cols, rows), jnp.bfloat16),
            pltpu.VMEM((2, count, cols, rows), jnp.bfloat16),
            pltpu.VMEM((2, bunch, step_j, channels), jnp.bfloat16),
            pltpu.VMEM((2, bunch, step_j, channels), jnp.float32),
            pltpu.VMEM((count // pieces, 2, cols, rows), jnp.float32),
            dma((3,)),
        ]
        + [dma((pieces,))] * 8
        + [dma((2,)), dma((9,)), dma((2,)), dma((2,))],
        compiler_params=pltpu.CompilerParams(
            collective_id=0, has_side_effects=True, vmem_limit_bytes=63 * 1024 * 1024
        ),
        name="exchange",
    )(pair, gain[None], shift[None], gw, gb[None], left, right)


PITCH = 33


def polish_kernel(gate_ref, og_ref, os_ref, ow_ref, ob_ref, tri_ref, out, held, done):
    rows, step_j, channels = gate_ref.shape
    hidden = tri_ref.shape[0]
    tiles, lanes = held.shape[0], held.shape[2]
    group = 16
    for tile in range(tiles):
        cut = slice(tile * lanes, (tile + 1) * lanes)

        def block(g):
            return tri_ref[pl.ds(g * group, group), :, cut].astype(jnp.float32)

        zero = jnp.zeros((step_j, lanes), jnp.float32)
        first = tri_ref[0, :, cut].astype(jnp.float32)

        def gauge(g, sums):
            moved = block(g) - first[None]
            return sums[0] + jnp.sum(moved, axis=0), sums[1] + jnp.sum(moved * moved, axis=0)

        total, power = lax.fori_loop(0, hidden // group, gauge, (zero, zero), unroll=STATS_UNROLL)
        shift = total / hidden
        centre = first + shift
        spread = jnp.maximum(power - total * shift, 0.0)
        scale = lax.rsqrt(spread / hidden + 1e-05)

        def normalise(g, _):
            for n in range(group):
                h = g * group + n
                value = (tri_ref[h, :, cut].astype(jnp.float32) - centre) * scale
                held[tile, pl.ds(h * PITCH, step_j), :] = value * og_ref[h] + os_ref[h]
            return 0

        lax.fori_loop(0, hidden // group, normalise, 0, unroll=NORM_UNROLL)

    def project(j, _):
        for tile in range(tiles):
            value = held[tile, pl.ds(j, hidden, stride=PITCH), :].astype(jnp.bfloat16)
            done[pl.ds(tile * lanes * PITCH + j, lanes, stride=PITCH), :] = lax.dot_general(
                value, ow_ref[...], (((0,), (0,)), ((), ())), preferred_element_type=jnp.float32
            )
        return 0

    lax.fori_loop(0, step_j, project, 0, unroll=PROJECT_UNROLL)
    bunch = 32

    def close(g, _):
        for n in range(bunch):
            at = g * bunch + n
            update = gate_ref[at] * (done[pl.ds(at * PITCH, step_j), :] + ob_ref[...])
            out[at] = update.astype(jnp.bfloat16)
        return 0

    lax.fori_loop(0, rows // bunch, close, 0)


def polish(gates, og, os, ow, ob, tri, step_j):
    rows, cols, channels = gates.shape
    hidden = tri.shape[0]
    lanes = 128 if rows % 128 == 0 else rows
    whole = lambda *shape: pl.BlockSpec(shape, lambda j: (0,) * len(shape))
    scalars = pl.BlockSpec(memory_space=pltpu.SMEM)
    moved = pl.BlockSpec((rows, step_j, channels), lambda j: (0, j, 0))
    return pl.pallas_call(
        polish_kernel,
        grid=(cols // step_j,),
        in_specs=[
            moved,
            scalars,
            scalars,
            whole(hidden, channels),
            whole(1, channels),
            pl.BlockSpec((hidden, step_j, rows), lambda j: (0, j, 0)),
        ],
        out_specs=moved,
        out_shape=jax.ShapeDtypeStruct((rows, cols, channels), jnp.bfloat16),
        scratch_shapes=[
            pltpu.VMEM((rows // lanes, hidden * PITCH, lanes), jnp.float32),
            pltpu.VMEM((rows * PITCH, channels), jnp.float32),
        ],
        compiler_params=pltpu.CompilerParams(vmem_limit_bytes=60 * 1024 * 1024),
        name="polish",
    )(gates, og, os, ow, ob[None], tri)


def spread_kernel(x_ref, gain_ref, shift_ref, w_ref, b_ref, left_ref, right_ref, flat, made):
    rows, step_k, channels = x_ref.shape
    count = left_ref.shape[0]
    tiles, _, lanes = made.shape
    tall = rows + 1
    bunch = rows // BUNCHES

    def normalise(g, _):
        normed = wide_norm(x_ref[pl.ds(g * bunch, bunch)], gain_ref[...], shift_ref[...])
        for n in range(bunch):
            for k in range(0, step_k, 8):
                flat[pl.ds(k * tall + g * bunch + n, 8, stride=tall), :] = normed[n, k : k + 8]
        return 0

    lax.fori_loop(0, BUNCHES, normalise, 0)

    def mix(k, _):
        line = flat[pl.ds(k * tall, rows), :].astype(jnp.bfloat16)
        mixed = flipped_dot(w_ref[...], line) + b_ref[...]
        for side in range(2):
            base = 2 * side * count
            value = jax.nn.sigmoid(mixed[base : base + count]) * mixed[base + count : base + 2 * count]
            for tile in range(tiles):
                made[tile, pl.ds(side * count * PITCH + k, count, stride=PITCH), :] = value[
                    :, tile * lanes : (tile + 1) * lanes
                ]
        return 0

    lax.fori_loop(0, step_k, mix, 0, unroll=16)

    def put(h, _):
        for tile in range(tiles):
            cut = slice(tile * lanes, (tile + 1) * lanes)
            for side, out in enumerate((left_ref, right_ref)):
                out[h, :, cut] = made[
                    tile, pl.ds((side * count + h) * PITCH, step_k), :
                ].astype(jnp.bfloat16)
        return 0

    lax.fori_loop(0, count, put, 0, unroll=4)


def project_pair(pair, gain, shift, weight, bias, step_k):
    rows, cols, channels = pair.shape
    count = weight.shape[0] // 4
    lanes = 128 if rows % 128 == 0 else rows
    whole = lambda *shape: pl.BlockSpec(shape, lambda k: (0,) * len(shape))
    return pl.pallas_call(
        spread_kernel,
        grid=(cols // step_k,),
        in_specs=[
            pl.BlockSpec((rows, step_k, channels), lambda k: (0, k, 0)),
            whole(1, channels),
            whole(1, channels),
            whole(4 * count, channels),
            whole(4 * count, 1),
        ],
        out_specs=[pl.BlockSpec((count, step_k, rows), lambda k: (0, k, 0))] * 2,
        out_shape=[jax.ShapeDtypeStruct((count, cols, rows), jnp.bfloat16)] * 2,
        scratch_shapes=[
            pltpu.VMEM((step_k * (rows + 1), channels), jnp.float32),
            pltpu.VMEM((rows // lanes, 2 * count * PITCH, lanes), jnp.float32),
        ],
        compiler_params=pltpu.CompilerParams(vmem_limit_bytes=60 * 1024 * 1024),
        name="project",
    )(pair, gain[None], shift[None], weight, bias[:, None])


def swap(value, axis, bit):
    count = lax.axis_size(axis)
    return lax.ppermute(value, axis, [(n, n ^ bit) for n in range(count)])


def pick(first_mine, mine, other):
    return jnp.where(first_mine, mine, other), jnp.where(first_mine, other, mine)


def cross_term(lefts, far, chunk, contract):
    left_far, (_, near), (_, beyond) = far[chunk]
    return (contract(near, lefts[chunk]) + contract(beyond, left_far)).astype(jnp.bfloat16)


def per_device_kernel(
    pair,
    ln_gain,
    ln_shift,
    proj_weight,
    proj_bias,
    gate_weight,
    gate_bias,
    out_gain,
    out_shift,
    out_weight,
    out_bias,
):
    depth_n = lax.axis_size("depth")
    depth = lax.axis_index("depth")
    rows, cols, channels = pair.shape
    hidden = proj_weight.shape[1] // 4
    per_depth = hidden // depth_n
    step, wide = 16, PITCH - 1
    weight = proj_weight.T.reshape(4, hidden, channels)
    bias = proj_bias.reshape(4, hidden)
    mine = lax.dynamic_slice_in_dim(weight, depth * per_depth, per_depth, 1)
    mine_bias = lax.dynamic_slice_in_dim(bias, depth * per_depth, per_depth, 1)
    left, right = project_pair(
        pair, ln_gain, ln_shift, mine.reshape(-1, channels), mine_bias.reshape(-1), wide
    )
    triangle, gates = exchange(
        pair, ln_gain, ln_shift, gate_weight, gate_bias, left, right, PIECES, step
    )
    triangle = triangle.reshape(hidden, cols, rows)
    return polish(gates, out_gain, out_shift, out_weight, out_bias, triangle, wide)


def per_device(
    pair,
    ln_gain,
    ln_shift,
    proj_weight,
    proj_bias,
    gate_weight,
    gate_bias,
    out_gain,
    out_shift,
    out_weight,
    out_bias,
):
    rows_n, cols_n, depth_n = (lax.axis_size(a) for a in ("row", "col", "depth"))
    row, col, depth = (lax.axis_index(a) for a in ("row", "col", "depth"))
    rows, cols, channels = pair.shape
    hidden = proj_weight.shape[1] // 4
    low, high = col % 2, col // 2
    core = depth % 2
    per_depth = hidden // depth_n
    per_col = per_depth // 2
    step = per_col // CHUNKS
    half_j = 2 * cols
    part = cols // 2

    weight = proj_weight.T.reshape(4, hidden, channels)
    bias = proj_bias.reshape(4, hidden)
    first = depth * per_depth
    mine = lax.dynamic_slice_in_dim(weight, first, per_depth, 1)
    mine_bias = lax.dynamic_slice_in_dim(bias, first, per_depth, 1)
    mine = jnp.where(low == 0, mine, jnp.roll(mine, per_col, 1))
    mine_bias = jnp.where(low == 0, mine_bias, jnp.roll(mine_bias, per_col, 1))
    step_k = 16
    made = project_all(
        pair, ln_gain, ln_shift, mine.reshape(-1, channels), mine_bias.reshape(-1), 2 * CHUNKS, step_k
    )
    lefts, rights = made[: 2 * CHUNKS], made[2 * CHUNKS :]

    def gather_rows(right):
        if rows_n == 2:
            return pick(row == high, right, swap(right, "row", 1))
        whole = lax.all_gather(right, "row", axis=2, tiled=True)
        return (
            lax.dynamic_slice_in_dim(whole, high * half_j, half_j, 2),
            lax.dynamic_slice_in_dim(whole, (1 - high) * half_j, half_j, 2),
        )

    def contract(right, left):
        return jnp.einsum("hkj,hki->hji", right, left, preferred_element_type=jnp.float32)

    gathered = []
    far, crossed = [], []
    for chunk in range(CHUNKS):
        ahead = (lefts[CHUNKS + chunk], rights[CHUNKS + chunk])
        if chunk >= 2:
            *ahead, crossed[chunk - 2] = lax.optimization_barrier((*ahead, crossed[chunk - 2]))
        left_far, right_far = (swap(value, "col", 1) for value in ahead)
        far.append((left_far, gather_rows(rights[chunk]), gather_rows(right_far)))
        if chunk >= 1:
            crossed.append(cross_term(lefts, far, chunk - 1, contract))
    crossed.append(cross_term(lefts, far, CHUNKS - 1, contract))
    for chunk in range(CHUNKS):
        left_near = lefts[chunk]
        left_far, (near_own, _), (far_own, _) = far[chunk]
        arrived = swap(crossed[chunk], "col", 2)
        own = contract(near_own, left_near) + contract(far_own, left_far)
        triangle = (own + arrived.astype(jnp.float32)).astype(jnp.bfloat16)
        keep = lax.dynamic_slice_in_dim(triangle, low * cols, cols, 1)
        give = lax.dynamic_slice_in_dim(triangle, (1 - low) * cols, cols, 1)
        block = jnp.concatenate([keep, swap(give, "col", 1)], axis=0)
        same = lax.dynamic_slice_in_dim(block, core * part, part, 1)
        across = lax.dynamic_slice_in_dim(block, (1 - core) * part, part, 1)
        gathered += [
            same,
            swap(across, "depth", 1),
            swap(same, "depth", 2),
            swap(across, "depth", 3),
        ]

    order = jnp.concatenate(
        [
            (depth ^ m) * per_depth + (low ^ n) * per_col + chunk * step + jnp.arange(step)
            for chunk in range(CHUNKS)
            for m in range(4)
            for n in range(2)
        ]
    )
    finished = finish_all(
        pair,
        core,
        part,
        ln_gain,
        ln_shift,
        gate_weight,
        gate_bias,
        out_gain[order],
        out_shift[order],
        out_weight[order],
        out_bias,
        gathered,
        step_k,
    )
    first, second = pick(core == 0, finished, swap(finished, "depth", 1))
    return jnp.concatenate([first, second], axis=1)


def solution(mesh):
    placed = (P("row", "col", None), P(), P(), P(), P(), P(), P(), P(), P(), P(), P())
    small = tuple(mesh.shape[a] for a in ("row", "col", "depth")) == (2, 4, 4)
    return jax.shard_map(
        per_device_kernel if small else per_device, mesh=mesh, in_specs=placed, out_specs=P("row", "col", None), check_vma=False
    )
```
